128 devices in a mesh: dp: 16 (over y_lo, z, core), space: 8 (over y_hi, x).
Axes of the slice: x: 4, y: 4 (y_hi: 2, y_lo: 2; y = y_hi * 2 + y_lo), z: 4, core: 2. Of those that a mesh axis runs over, the one named last changes fastest.
Arguments:
- volume: bfloat16 [16, 32, 32, 32, 128], P('dp', 'space'), may hold values from -6 to 6
- kernel: bfloat16 [3, 3, 3, 128, 256], replicated, may hold values from -0.109375 to 0.109375
- cotangent: bfloat16 [16, 16, 16, 16, 256], P('dp', 'space'), may hold values from -6 to 6
Outputs:
- switched: bfloat16 [16, 256, 4096], P('dp', 'space')
- volume_grad: bfloat16 [16, 32, 32, 32, 128], P('dp', 'space')
- kernel_grad: float32 [3, 3, 3, 128, 256], P(None, None, None, 'dp')
The draws below stay inside these ranges and needn't reach their ends.
All inputs are finite; a program needn't handle non-finite values.
Results may differ from the reference program's by a relative error of at most 0.0049.
Values may be sent and summed in bfloat16 or wider, within the bound.
A program may use at most 64 MiB of HBM per device.

```python
import math
import jax
import jax.numpy as jnp
from jax import lax

CIN = 128
COUT = 256
SIDE = 32
SAMPLES = 16
DEPTH = 32
D2 = 16
S2 = 16


def raised(drawn, rng, source, target, parts, factor):
    def block_of(position):
        return (jnp.arange(drawn.shape[position]) // (drawn.shape[position] // parts)).reshape((-1,) + (1,) * (drawn.ndim - 1 - position))

    near = jax.random.permutation(rng, parts)[block_of(target)]
    other_side = (block_of(target) + parts // 2) % parts
    return jnp.where((block_of(source) == near) | (block_of(source) == other_side), factor * drawn, drawn)


def steps_of(stream_key, shape, pieces, low, largest):
    def one(position, parts):
        steps = jax.random.uniform(jax.random.fold_in(jax.random.fold_in(stream_key, 6), position), (parts,), jnp.float32, low / len(pieces), largest / len(pieces))
        return jnp.repeat(jnp.exp(steps), shape[position] // parts).reshape((-1,) + (1,) * (len(shape) - position - 1))

    level = one(*pieces[0])
    for cut in pieces[1:]:
        level = level * one(*cut)
    return level


def noise(stream_key, dims, spread, reach, pieces=(), kind=jnp.bfloat16):
    gain = steps_of(stream_key, dims, pieces, -0.22, 0.18) if pieces else 1.0
    array = jax.random.normal(stream_key, dims, jnp.float32) * spread * gain
    return jnp.minimum(jnp.maximum(array, -reach), reach).astype(kind)


def bell_draw_with(key, extent, spread, bound, cuts, heavy, dtype=jnp.bfloat16):
    drawn = spread * jax.random.normal(key, extent, jnp.float32)
    if cuts:
        drawn = drawn * steps_of(key, extent, cuts, -0.22, 0.18)
    return jnp.clip(raised(drawn, jax.random.fold_in(key, 3), *heavy), -bound, bound).astype(dtype)


def setup_inputs(seed: int = 0) -> dict:
    key_list = jax.random.split(jax.random.key(seed), 4)
    return {
        "volume": bell_draw_with(key_list[0], (SAMPLES, DEPTH, SIDE, SIDE, CIN), 1.0, 6.0, ((0, 16), (1, 8)), (0, 4, 16, 2.0)),
        "kernel": noise(key_list[1], (3, 3, 3, CIN, COUT), (27 * CIN) ** -0.5, 0.109375),
        "cotangent": noise(key_list[2], (SAMPLES, D2, S2, S2, COUT), 1.0, 6.0, ((0, 16), (1, 8))),
    }


def forward_conv(volume_one, kernel):
    return lax.conv_general_dilated(volume_one, kernel, (2, 2, 2), ((1, 1), (1, 1), (1, 1)), dimension_numbers=('NDHWC', 'DHWIO', 'NDHWC'), preferred_element_type=jnp.float32)

def one_sample(volume_one, kernel, cotangent_one):
    preact = forward_conv(volume_one, kernel)
    sigmoid_z = jax.nn.sigmoid(preact)
    activated = (preact * sigmoid_z).astype(jnp.bfloat16)
    slope = sigmoid_z * (1.0 + preact * (1.0 - sigmoid_z))
    grad_pre = (cotangent_one.astype(jnp.float32) * slope).astype(jnp.bfloat16)
    flipped = kernel[::-1, ::-1, ::-1]
    data_grad = lax.conv_general_dilated(grad_pre, flipped, (1, 1, 1), ((1, 2), (1, 2), (1, 2)), lhs_dilation=(2, 2, 2), dimension_numbers=('NDHWC', 'DHWOI', 'NDHWC'), preferred_element_type=jnp.float32).astype(jnp.bfloat16)
    kernel_part = lax.conv_general_dilated(volume_one, grad_pre, (1, 1, 1), ((1, 0), (1, 0), (1, 0)), rhs_dilation=(2, 2, 2), dimension_numbers=('CDHWN', 'IDHWO', 'DHWNC'), preferred_element_type=jnp.float32)
    return (activated, data_grad, kernel_part)

def reference(volume, kernel, cotangent):

    def step(total, pair):
        activated, data_grad, kernel_part = one_sample(pair[0][None], kernel, pair[1][None])
        return (total + kernel_part, (activated[0], data_grad[0]))
    start = jnp.zeros((3, 3, 3, volume.shape[4], kernel.shape[4]), jnp.float32)
    total, outs = lax.scan(step, start, (volume, cotangent))
    activated, volume_grad = outs
    samples, planes, rows, cols, chans = activated.shape
    switched = jnp.transpose(activated, (0, 4, 1, 2, 3)).reshape(samples, chans, planes * rows * cols)
    scale = 1.0 / math.sqrt(samples * planes * rows * cols)
    return (switched, volume_grad, total * scale)
```

```python
import functools

import jax
import jax.numpy as jnp
from jax import lax
from jax.experimental import pallas as pl
from jax.experimental.pallas import tpu as pltpu
from jax.sharding import PartitionSpec as P

MESH = pl.DeviceIdType.MESH
BF, F32 = jnp.bfloat16, jnp.float32
NT = (((1,), (1,)), ((), ()))
TAPS = 9
PAIRS = {0: ((1, 1), (3, 2)), 1: ((0, 0), (2, 1)), 2: ((1, 0), (3, 1))}
REACH = {0: ((0, 1),), 1: ((0, 2), (1, 0)), 2: ((1, 1),), 3: ((1, 2), (2, 0))}


def nt(a, b):
    return lax.dot_general(a, b, NT, preferred_element_type=F32)


def mm(a, b):
    return jnp.dot(a, b, preferred_element_type=F32)


def kernel(
    scale,
    vol_hbm, w_hbm, ct_hbm,
    sw_ref, vg_ref, kg_ref,
    vol, w, ct, spread, taps, tt, ttr, gp, gps, gpr, hs, hr, swb, fine,
    o1, w1, c1, o2, w2, c2, o3, w3, c3,
    in_sem, pair_ss, pair_rs, halo_ss, halo_rs, sw_ss, sw_rs, red_ss, red_rs,
):
    dp, sp = lax.axis_index("dp"), lax.axis_index("space")
    core, z, y, x = dp % 2, (dp // 2) % 4, (sp // 4) * 2 + dp // 8, sp % 4

    def chip(x, y, z, core):
        return ((y % 2) * 8 + z * 2 + core, (y // 2) * 4 + x)

    partner = chip(x, y, z, 1 - core)
    along = {
        "z": [chip(x, y, (z + j) % 4, core) for j in (1, 2, 3)],
        "y": [chip(x, (y + j) % 4, z, core) for j in (1, 2, 3)],
        "x": [chip((x + j) % 4, y, z, core) for j in (1, 2, 3)],
    }
    slabs = [(dp, (sp + j) % 8) for j in range(1, 8)]

    def remote(src, dst, ss, rs, to):
        return pltpu.make_async_remote_copy(
            src_ref=src, dst_ref=dst, send_sem=ss, recv_sem=rs, device_id=to, device_id_type=MESH
        )

    loads = {}
    for i, p in enumerate((3, 1, 2, 0)):
        loads["v", p] = pltpu.make_async_copy(vol_hbm.at[p], vol.at[p], in_sem.at[i])
    for kd in range(3):
        rows = pl.ds(kd * 1152, 1152)
        loads["w", kd] = pltpu.make_async_copy(w_hbm.at[rows], w.at[rows], in_sem.at[4 + kd])
    loads["c"] = pltpu.make_async_copy(ct_hbm, ct, in_sem.at[7])
    for which in (("v", 3), ("w", 0), ("v", 1), ("v", 2), ("w", 1), ("w", 2), ("v", 0), "c"):
        loads[which].start()

    barrier = pltpu.get_barrier_semaphore()
    peers = [partner, *along["z"], along["y"][0], along["y"][2], *slabs]
    for peer in peers:
        pl.semaphore_signal(barrier, inc=1, device_id=peer, device_id_type=MESH)

    def edge(condition, ref):
        @pl.when(condition)
        def _():
            ref[...] = jnp.zeros(ref.shape, ref.dtype)

    edge(sp == 7, gp.at[2])
    edge(sp == 0, hr)

    first_column = lax.broadcasted_iota(jnp.int32, (512, 128), 0) % 16 == 0
    last_column = lax.broadcasted_iota(jnp.int32, (256, 256), 0) % 16 == 15

    def unfold(p):
        loads["v", p].wait()
        spread[pl.ds(8, 1024)] = vol[p].astype(F32)
        even = spread[pl.ds(8, 512, stride=2)].astype(BF)
        odd = spread[pl.ds(9, 512, stride=2)].astype(BF)
        left = jnp.where(first_column, 0.0, spread[pl.ds(7, 512, stride=2)]).astype(BF)
        for kw, source in enumerate((left, even, odd)):
            rows = source.reshape(16, 32, 128)
            upper, lower = rows[:, :16], rows[:, 16:]
            before = jnp.concatenate([jnp.zeros((1, 16, 128), BF), lower[:-1]], axis=0)
            for kh, block in enumerate((before, upper, lower)):
                at = (kh * 3 + kw) * 128
                taps[p, :, at : at + 128] = block.reshape(256, 128)

    row = lax.broadcasted_iota(jnp.int32, (128, 128), 0)
    column = lax.broadcasted_iota(jnp.int32, (128, 128), 1)
    channel = (((row % 64) // 8) * 2 + row // 64) * 8 + row % 8
    sort = (column == channel).astype(F32).astype(BF)

    def turn(p):
        for t in range(TAPS):
            turned = nt(sort, taps[p, :, t * 128 : (t + 1) * 128]).astype(BF)
            tt[0, p, t * 64 : (t + 1) * 64] = turned[:64]
            tt[1, p, t * 64 : (t + 1) * 64] = turned[64:]

    spread[0:8] = jnp.zeros((8, 128), F32)
    unfold(3)
    loads["w", 0].wait()
    hs[...] = mm(taps[3], w[0:1152]).astype(BF)
    pl.semaphore_wait(barrier, len(peers))
    halo = remote(hs, hr, halo_ss.at[0], halo_rs.at[0], (dp, (sp + 1) % 8))

    @pl.when(sp < 7)
    def _():
        halo.start()

    unfold(1)
    unfold(2)
    loads["w", 1].wait()
    loads["w", 2].wait()
    pre1 = mm(taps[1], w[0:1152]) + mm(taps[2], w[1152:2304]) + mm(taps[3], w[2304:3456])

    er = lax.broadcasted_iota(jnp.int32, (256, 256), 0)
    ec = lax.broadcasted_iota(jnp.int32, (256, 256), 1)
    unit = (er == ec).astype(F32).astype(BF)

    def share(o):
        return remote(gp.at[o], gpr.at[o], pair_ss.at[4 + o], pair_rs.at[4 + o], partner)

    def to_right(o):
        value = gp[o].astype(F32)
        gps[o] = jnp.where(last_column, 0.0, pltpu.roll(value, 255, 0)).astype(BF)

    def finish(o, v):
        s = jax.nn.sigmoid(v)
        slope = s * (1.0 + v * (1.0 - s))
        rows = pl.ds(o * 256, 256)
        gp[o] = (ct[rows].astype(F32) * slope).astype(BF)
        return (v * s).astype(BF)

    loads["c"].wait()
    act1 = finish(1, pre1)
    share(1).start()
    to_right(1)

    unfold(0)
    pre0 = mm(taps[0], w[1152:2304]) + mm(taps[1], w[2304:3456])
    pairs = []
    for p in (0, 1, 2, 3):
        turn(p)
        pairs.append(remote(tt.at[1 - core, p], ttr.at[p], pair_ss.at[p], pair_rs.at[p], partner))
        pairs[-1].start()
    swb[:, 256:512] = nt(unit, act1).astype(BF)

    def grad_plane(p):
        for half, moves in ((0, ((1, 0),)), (1, ((2, 0), (0, 1)))):
            lhs, lhs_right, rhs, rhs_right = [], [], [], []
            for o, kd in REACH[p]:
                for kh, down in moves:
                    for source, out in ((gp, lhs), (gps, lhs_right)):
                        value = source[o]
                        if down:
                            value = jnp.concatenate([value[16:], jnp.zeros((16, 256), BF)], axis=0)
                        out.append(value)
                    at = (kd * 9 + kh * 3) * 128
                    rhs_right.append(w[at : at + 128])
                    rhs.append(w[at + 128 : at + 384])
            both = nt(jnp.concatenate(lhs, axis=1), jnp.concatenate(rhs, axis=1))
            more = nt(jnp.concatenate(lhs_right, axis=1), jnp.concatenate(rhs_right, axis=1))
            fine[:, pl.ds(half * 32, 16, stride=2), :] = both[:, :128].reshape(16, 16, 128)
            fine[:, pl.ds(half * 32 + 1, 16, stride=2), :] = (both[:, 128:] + more).reshape(16, 16, 128)
        vg_ref[p] = fine[...].reshape(1024, 128).astype(BF)

    grad_plane(2)

    @pl.when(sp > 0)
    def _():
        halo.wait_recv()

    act0 = finish(0, pre0 + hr[...].astype(F32))
    share(0).start()
    back = remote(gp.at[0], gp.at[2], halo_ss.at[1], halo_rs.at[1], (dp, (sp + 7) % 8))

    @pl.when(sp > 0)
    def _():
        back.start()

    def own_part(kd):
        (a, oa), (b, ob) = PAIRS[kd]
        lhs = jnp.concatenate([tt[core, a], tt[core, b]], axis=1)
        return mm(lhs, jnp.concatenate([gp[oa], gp[ob]], axis=0))

    def pair_part(kd):
        (a, oa), (b, ob) = PAIRS[kd]
        lhs = jnp.concatenate([ttr[a], ttr[b]], axis=1)
        return mm(lhs, jnp.concatenate([gpr[oa], gpr[ob]], axis=0))

    def put1(kd, total):
        for t in range(TAPS):
            for group in range(8):
                block = total[t * 64 + group * 8 : t * 64 + group * 8 + 8]
                tile = jnp.concatenate([block[:, :128], block[:, 128:]], axis=0)
                o1[kd, group % 4, (group // 4) * 9 + t] = tile
                w1[kd, group % 4, (group // 4) * 9 + t] = tile.astype(BF)

    def copies(kd, stage):
        out = []
        for j in range(3):
            at = (kd * 3 + stage) * 3 + j
            if stage == 0:
                src, dst, to = w1.at[kd, (z + j + 1) % 4], c1.at[kd, j], along["z"][j]
            elif stage == 1:
                src, dst, to = w2.at[kd, (y + j + 1) % 2], c2.at[kd, j], along["y"][j]
            else:
                src, dst, to = w3.at[kd], c3.at[kd, j], along["x"][j]
            out.append(remote(src, dst, red_ss.at[at], red_rs.at[at], to))
        return out

    def send(kd, stage):
        for c in copies(kd, stage):
            c.start()

    def arrive(kd, stage):
        for c in copies(kd, stage):
            c.wait_recv()

    def summed(own, got):
        return own + got[0].astype(F32) + got[1].astype(F32) + got[2].astype(F32)

    def step1(kd):
        arrive(kd, 0)
        total = summed(o1[kd, z], c1.at[kd]).reshape(2, 9, 16, 128)
        o2[kd] = total
        w2[kd] = total.astype(BF)
        send(kd, 1)

    def step2(kd):
        arrive(kd, 1)
        total = summed(o2[kd, y % 2], c2.at[kd])
        o3[kd] = total
        w3[kd] = total.astype(BF)
        send(kd, 2)

    def step3(kd):
        arrive(kd, 2)
        total = summed(o3[kd], c3.at[kd]) * scale
        for t in range(TAPS):
            at = (kd * 9 + t) * 8
            kg_ref[at : at + 8, 0:128] = total[t, 0:8]
            kg_ref[at : at + 8, 128:256] = total[t, 8:16]

    part1, part2 = own_part(1), own_part(2)
    for c in pairs:
        c.wait_recv()
    share(1).wait_recv()
    share(0).wait_recv()
    put1(1, part1 + pair_part(1))
    send(1, 0)
    put1(2, part2 + pair_part(2))
    send(2, 0)

    swb[:, 0:256] = nt(unit, act0).astype(BF)
    columns = pl.ds(pl.multiple_of(sp * 512, 512), 512)
    switches = []
    for j, to in enumerate(slabs):
        rows = pl.ds(pl.multiple_of(to[1] * 32, 32), 32)
        switches.append(remote(swb.at[rows], sw_ref.at[:, columns], sw_ss.at[j], sw_rs.at[j], to))
        switches[-1].start()
    sw_ref[:, columns] = swb[pl.ds(pl.multiple_of(sp * 32, 32), 32)]
    to_right(0)
    grad_plane(0)

    @pl.when(sp < 7)
    def _():
        back.wait_recv()

    share(2).start()
    part0 = own_part(0)
    step1(1)
    share(2).wait_recv()
    put1(0, part0 + pair_part(0))
    send(0, 0)
    step1(2)
    to_right(2)
    grad_plane(1)
    step2(1)
    step2(2)
    grad_plane(3)
    step1(0)
    step3(1)
    step2(0)
    step3(2)
    step3(0)

    for c in switches:
        c.wait()
    for c in pairs:
        c.wait_send()
    for o in range(3):
        share(o).wait_send()
    for kd in range(3):
        for stage in range(3):
            for c in copies(kd, stage):
                c.wait_send()

    @pl.when(sp < 7)
    def _():
        halo.wait_send()

    @pl.when(sp > 0)
    def _():
        back.wait_send()


def body(volume, weights, cotangent):
    count = 16 * 16 * 16 * 16
    vmem = functools.partial(pltpu.VMEM)
    dma = pltpu.SemaphoreType.DMA
    whole = pl.BlockSpec(memory_space=pltpu.VMEM)
    switched, volume_grad, kernel_grad = pl.pallas_call(
        functools.partial(kernel, 1.0 / count**0.5),
        out_shape=(
            jax.ShapeDtypeStruct((32, 4096), BF),
            jax.ShapeDtypeStruct((4, 1024, 128), BF),
            jax.ShapeDtypeStruct((216, 256), F32),
        ),
        in_specs=[pl.BlockSpec(memory_space=pl.ANY)] * 3,
        out_specs=(whole, whole, whole),
        scratch_shapes=[
            vmem((4, 1024, 128), BF),
            vmem((3456, 256), BF),
            vmem((512, 256), BF),
            vmem((1040, 128), F32),
            vmem((4, 256, 1152), BF),
            vmem((2, 4, 576, 256), BF),
            vmem((4, 576, 256), BF),
            vmem((3, 256, 256), BF),
            vmem((3, 256, 256), BF),
            vmem((3, 256, 256), BF),
            vmem((256, 256), BF),
            vmem((256, 256), BF),
            vmem((256, 512), BF),
            vmem((16, 64, 128), F32),
            vmem((3, 4, 18, 16, 128), F32),
            vmem((3, 4, 18, 16, 128), BF),
            vmem((3, 3, 18, 16, 128), BF),
            vmem((3, 2, 9, 16, 128), F32),
            vmem((3, 2, 9, 16, 128), BF),
            vmem((3, 3, 9, 16, 128), BF),
            vmem((3, 9, 16, 128), F32),
            vmem((3, 9, 16, 128), BF),
            vmem((3, 3, 9, 16, 128), BF),
            dma((8,)),
            dma((7,)),
            dma((7,)),
            dma((2,)),
            dma((2,)),
            dma((7,)),
            dma((7,)),
            dma((27,)),
            dma((27,)),
        ],
        compiler_params=pltpu.CompilerParams(
            collective_id=0, has_side_effects=True, vmem_limit_bytes=56 * 2**20
        ),
        name="conv_step",
    )(
        volume.reshape(4, 1024, 128),
        weights.reshape(3456, 256),
        cotangent.reshape(512, 256),
    )
    return (
        switched[None],
        volume_grad.reshape(1, 4, 32, 32, 128),
        kernel_grad.reshape(3, 3, 3, 8, 256),
    )


def solution(mesh):
    in_specs = (P("dp", "space", None, None, None), P(), P("dp", "space", None, None, None))
    out_specs = (
        P("dp", "space", None),
        P("dp", "space", None, None, None),
        P(None, None, None, "dp", None),
    )
    return jax.shard_map(body, mesh=mesh, in_specs=in_specs, out_specs=out_specs, check_vma=False)
```

```python
import functools

import jax
import jax.numpy as jnp
from jax import lax
from jax.experimental import pallas as pl
from jax.experimental.pallas import tpu as pltpu
from jax.sharding import PartitionSpec as P

MESH = pl.DeviceIdType.MESH
BF, F32 = jnp.bfloat16, jnp.float32
NT = (((1,), (1,)), ((), ()))
TAPS = 9
PAIRS = {0: ((1, 1), (3, 2)), 1: ((0, 0), (2, 1)), 2: ((1, 0), (3, 1))}
REACH = {0: ((0, 1),), 1: ((0, 2), (1, 0)), 2: ((1, 1),), 3: ((1, 2), (2, 0))}


def nt(a, b):
    return lax.dot_general(a, b, NT, preferred_element_type=F32)


def mm(a, b):
    return jnp.dot(a, b, preferred_element_type=F32)


class Part:
    def __init__(self, kd, low, count, order):
        self.kd, self.low, self.count, self.order = kd, low, count, order
        self.half = (count + 1) // 2
        if order == "z":
            self.sizes = ((4, 2 * count), (2, count), (1, count))
        else:
            self.sizes = ((4, 4 * self.half), (4, self.half), (1, self.half))
        self.copies = 9 if order == "z" else 10

    def scratch(self):
        shapes = []
        for blocks, tiles in self.sizes:
            shapes.append(pltpu.VMEM((blocks, tiles, 16, 128), F32))
            shapes.append(pltpu.VMEM((blocks, tiles, 16, 128), BF))
            shapes.append(pltpu.VMEM((3, tiles, 16, 128), BF))
        if self.order == "y":
            shapes += [pltpu.VMEM((self.half, 16, 128), F32)] * 2
        return shapes


PARTS = (Part(1, 0, 9, "z"), Part(2, 0, 9, "y"), Part(0, 0, 5, "z"), Part(0, 5, 4, "y"))
SUMS = sum(part.copies for part in PARTS)


def kernel(scale, vol_hbm, w_hbm, ct_hbm, sw_ref, vg_ref, kg_ref, *rest):
    (
        vol, w, ct, spread, taps, tt, ttr, gp, gps, gpr, hs, hr, ps, pr, cr, swb, fine,
        in_sem, pair_ss, pair_rs, edge_ss, edge_rs, sw_ss, sw_rs, sum_ss, sum_rs, ready,
    ) = rest[:27]
    rest, room, number = list(rest[27:]), {}, {}
    for i, part in enumerate(PARTS):
        count = len(part.scratch())
        room[i], rest = rest[:count], rest[count:]
        number[i] = sum(p.copies for p in PARTS[:i])

    dp, sp = lax.axis_index("dp"), lax.axis_index("space")
    core, z, y, x = dp % 2, (dp // 2) % 4, (sp // 4) * 2 + dp // 8, sp % 4
    y_hi = sp // 4

    def chip(x, y, z, core):
        return ((y % 2) * 8 + z * 2 + core, (y // 2) * 4 + x)

    partner = chip(x, y, z, 1 - core)
    along = {
        "z": [chip(x, y, (z + j) % 4, core) for j in (1, 2, 3)],
        "y": [chip(x, (y + j) % 4, z, core) for j in (1, 2, 3)],
        "x": [chip((x + j) % 4, y, z, core) for j in (1, 2, 3)],
    }
    slabs = [(dp, (sp + j) % 8) for j in range(1, 8)]
    above, below = (dp, (sp + 1) % 8), (dp, (sp + 7) % 8)

    def remote(src, dst, ss, rs, to):
        return pltpu.make_async_remote_copy(
            src_ref=src, dst_ref=dst, send_sem=ss, recv_sem=rs, device_id=to, device_id_type=MESH
        )

    def signal(sem, to):
        pl.semaphore_signal(sem, inc=1, device_id=to, device_id_type=MESH)

    loads = {}
    for i, p in enumerate((3, 0, 1, 2)):
        loads["v", p] = pltpu.make_async_copy(vol_hbm.at[p], vol.at[p], in_sem.at[i])
    for kd in range(3):
        rows = pl.ds(kd * 1152, 1152)
        loads["w", kd] = pltpu.make_async_copy(w_hbm.at[rows], w.at[rows], in_sem.at[4 + kd])
    loads["c"] = pltpu.make_async_copy(ct_hbm, ct, in_sem.at[7])
    for which in (("v", 3), ("w", 0), ("v", 0), ("v", 1), ("w", 1), ("w", 2), ("v", 2), "c"):
        loads[which].start()

    barrier = pltpu.get_barrier_semaphore()
    near = [along[axis][j] for axis in "xyz" for j in (0, 2)]
    for peer in [partner, *near]:
        signal(barrier, peer)

    @pl.when(sp == 3)
    def _():
        signal(barrier, above)

    @pl.when(sp == 4)
    def _():
        signal(barrier, below)

    def edge(condition, ref):
        @pl.when(condition)
        def _():
            ref[...] = jnp.zeros(ref.shape, ref.dtype)

    edge(sp == 7, gp.at[2])
    edge(sp == 0, hr)

    first_column = lax.broadcasted_iota(jnp.int32, (512, 128), 0) % 16 == 0
    last_column = lax.broadcasted_iota(jnp.int32, (256, 256), 0) % 16 == 15

    def unfold(p):
        loads["v", p].wait()
        spread[pl.ds(8, 1024)] = vol[p].astype(F32)
        even = spread[pl.ds(8, 512, stride=2)].astype(BF)
        odd = spread[pl.ds(9, 512, stride=2)].astype(BF)
        left = jnp.where(first_column, 0.0, spread[pl.ds(7, 512, stride=2)]).astype(BF)
        for kw, source in enumerate((left, even, odd)):
            rows = source.reshape(16, 32, 128)
            upper, lower = rows[:, :16], rows[:, 16:]
            before = jnp.concatenate([jnp.zeros((1, 16, 128), BF), lower[:-1]], axis=0)
            for kh, block in enumerate((before, upper, lower)):
                at = (kh * 3 + kw) * 128
                taps[p, :, at : at + 128] = block.reshape(256, 128)

    row = lax.broadcasted_iota(jnp.int32, (128, 128), 0)
    column = lax.broadcasted_iota(jnp.int32, (128, 128), 1)
    channel = (((row % 64) // 8) * 2 + row // 64) * 8 + row % 8
    sort = (column == channel).astype(F32).astype(BF)
    pairs = []

    def turn(p):
        for t in range(TAPS):
            turned = nt(sort, taps[p, :, t * 128 : (t + 1) * 128]).astype(BF)
            tt[0, p, t * 64 : (t + 1) * 64] = turned[:64]
            tt[1, p, t * 64 : (t + 1) * 64] = turned[64:]
        pairs.append(remote(tt.at[1 - core, p], ttr.at[p], pair_ss.at[p], pair_rs.at[p], partner))
        pairs[-1].start()

    er = lax.broadcasted_iota(jnp.int32, (256, 256), 0)
    ec = lax.broadcasted_iota(jnp.int32, (256, 256), 1)
    unit = (er == ec).astype(F32).astype(BF)

    def share(o):
        return remote(gp.at[o], gpr.at[o], pair_ss.at[4 + o], pair_rs.at[4 + o], partner)

    def to_right(o):
        value = gp[o].astype(F32)
        gps[o] = jnp.where(last_column, 0.0, pltpu.roll(value, 255, 0)).astype(BF)

    def slope_of(v):
        s = jax.nn.sigmoid(v)
        return s, s * (1.0 + v * (1.0 - s))

    def finish(o, v):
        s, slope = slope_of(v)
        gp[o] = (ct[pl.ds(o * 256, 256)].astype(F32) * slope).astype(BF)
        swb[:, o * 256 : (o + 1) * 256] = nt(unit, (v * s).astype(BF)).astype(BF)

    def grad_plane(p):
        for half, moves in ((0, ((1, 0),)), (1, ((2, 0), (0, 1)))):
            lhs, lhs_right, rhs, rhs_right = [], [], [], []
            for o, kd in REACH[p]:
                for kh, down in moves:
                    for source, out in ((gp, lhs), (gps, lhs_right)):
                        value = source[o]
                        if down:
                            value = jnp.concatenate([value[16:], jnp.zeros((16, 256), BF)], axis=0)
                        out.append(value)
                    at = (kd * 9 + kh * 3) * 128
                    rhs_right.append(w[at : at + 128])
                    rhs.append(w[at + 128 : at + 384])
            both = nt(jnp.concatenate(lhs, axis=1), jnp.concatenate(rhs, axis=1))
            more = nt(jnp.concatenate(lhs_right, axis=1), jnp.concatenate(rhs_right, axis=1))
            fine[:, pl.ds(half * 32, 16, stride=2), :] = both[:, :128].reshape(16, 16, 128)
            fine[:, pl.ds(half * 32 + 1, 16, stride=2), :] = (both[:, 128:] + more).reshape(16, 16, 128)
        vg_ref[p] = fine[...].reshape(1024, 128).astype(BF)

    def own_part(kd):
        (a, oa), (b, ob) = PAIRS[kd]
        lhs = jnp.concatenate([tt[core, a], tt[core, b]], axis=1)
        return mm(lhs, jnp.concatenate([gp[oa], gp[ob]], axis=0))

    def pair_part(kd):
        (a, oa), (b, ob) = PAIRS[kd]
        lhs = jnp.concatenate([ttr[a], ttr[b]], axis=1)
        return mm(lhs, jnp.concatenate([gpr[oa], gpr[ob]], axis=0))

    def copies(i, stage):
        part, refs, out = PARTS[i], room[i], []
        if stage == 3:
            at = number[i] + 9
            return [remote(refs[9], refs[10], sum_ss.at[at], sum_rs.at[at], along["y"][1])]
        axis = ("zyx" if part.order == "z" else "yzx")[stage]
        mine = {"z": z, "y": y, "x": 0}[axis]
        blocks = part.sizes[stage][0]
        for j in range(3):
            at = number[i] + stage * 3 + j
            src = refs[3 * stage + 1].at[(mine + j + 1) % blocks]
            out.append(remote(src, refs[3 * stage + 2].at[j], sum_ss.at[at], sum_rs.at[at], along[axis][j]))
        return out

    def send(i, stage):
        for c in copies(i, stage):
            c.start()

    def put(i, total):
        part, refs = PARTS[i], room[i]

        def store(block, tile_at, tile):
            refs[0][block, tile_at] = tile
            refs[1][block, tile_at] = tile.astype(BF)

        for t in range(part.count):
            for group in range(8):
                at = (part.low + t) * 64 + group * 8
                tile = jnp.concatenate([total[at : at + 8, :128], total[at : at + 8, 128:]], axis=0)
                y_lo, to_z = group // 4, group % 4
                if part.order == "z":
                    store(to_z, y_lo * part.count + t, tile)
                else:
                    for upper in range(2):
                        k = t - upper * (part.count - part.half)
                        if 0 <= k < part.half:
                            store(upper * 2 + y_lo, to_z * part.half + k, tile)
        send(i, 0)

    def write(part, start, count, value):
        for t in range(count):
            at = pl.multiple_of((part.kd * 9 + part.low + start + t) * 8, 8)
            kg_ref[pl.ds(at, 8), 0:128] = value[t, 0:8]
            kg_ref[pl.ds(at, 8), 128:256] = value[t, 8:16]

    def step(i, stage):
        part, refs = PARTS[i], room[i]
        for c in copies(i, stage):
            c.wait_recv()
        if stage == 3:
            write(part, (1 - y_hi) * (part.count - part.half), part.half, refs[10][...])
            return
        own, _, got = refs[3 * stage : 3 * stage + 3]
        axis = ("zyx" if part.order == "z" else "yzx")[stage]
        mine = {"z": z, "y": y, "x": 0}[axis]
        total = own[mine % part.sizes[stage][0]]
        for j in range(3):
            total = total + got[j].astype(F32)
        if stage < 2:
            total = total.reshape(*part.sizes[stage + 1], 16, 128)
            refs[3 * stage + 3][...] = total
            refs[3 * stage + 4][...] = total.astype(BF)
            send(i, stage + 1)
        elif part.order == "z":
            write(part, 0, part.count, total * scale)
        else:
            refs[9][...] = total * scale
            send(i, 3)
            write(part, y_hi * (part.count - part.half), part.half, total * scale)

    spread[0:8] = jnp.zeros((8, 128), F32)
    unfold(3)
    loads["w", 0].wait()
    hs[...] = mm(taps[3], w[0:1152]).astype(BF)

    pl.semaphore_wait(barrier, 7 + jnp.where((sp == 3) | (sp == 4), 1, 0))
    halo = remote(hs, hr, edge_ss.at[0], edge_rs.at[0], above)
    slope_part = remote(ps, pr, edge_ss.at[1], edge_rs.at[1], below)
    slope_ct = remote(ct_hbm.at[pl.ds(0, 256)], cr, edge_ss.at[2], edge_rs.at[2], below)

    @pl.when(sp < 7)
    def _():
        halo.start()

    @pl.when(sp > 0)
    def _():
        slope_ct.start()

    for peer in near:
        signal(ready, peer)

    unfold(0)
    unfold(1)
    loads["w", 1].wait()
    loads["w", 2].wait()
    pre0 = mm(taps[0], w[1152:2304]) + mm(taps[1], w[2304:3456])
    ps[...] = pre0.astype(BF)

    @pl.when(sp > 0)
    def _():
        slope_part.start()

    turn(3)
    turn(1)
    turn(0)
    unfold(2)
    pre1 = mm(taps[1], w[0:1152]) + mm(taps[2], w[1152:2304]) + mm(taps[3], w[2304:3456])
    loads["c"].wait()
    finish(1, pre1)
    share(1).start()
    turn(2)
    to_right(1)

    @pl.when(sp > 0)
    def _():
        halo.wait_recv()

    finish(0, pre0 + hr[...].astype(F32))
    share(0).start()

    part1, part2 = own_part(1), own_part(2)
    for c in pairs:
        c.wait_recv()
    share(1).wait_recv()
    share(0).wait_recv()
    pl.semaphore_wait(ready, len(near))
    put(0, part1 + pair_part(1))
    put(1, part2 + pair_part(2))

    @pl.when(sp < 7)
    def _():
        slope_ct.wait_recv()
        slope_part.wait_recv()
        _, slope = slope_of(pr[...].astype(F32) + hs[...].astype(F32))
        gp[2] = (cr[...].astype(F32) * slope).astype(BF)

    share(2).start()
    part0 = own_part(0)
    grad_plane(2)
    share(2).wait_recv()
    total0 = part0 + pair_part(0)
    put(2, total0)
    put(3, total0)
    to_right(0)
    to_right(2)
    for p in (0, 1, 3):
        grad_plane(p)

    columns = pl.ds(pl.multiple_of(sp * 512, 512), 512)
    sw_ref[:, columns] = swb[pl.ds(pl.multiple_of(sp * 32, 32), 32)]
    step(0, 0)
    step(1, 0)
    step(2, 0)
    step(3, 0)
    switches = []
    for j, to in enumerate(slabs):
        rows = pl.ds(pl.multiple_of(to[1] * 32, 32), 32)
        switches.append(remote(swb.at[rows], sw_ref.at[:, columns], sw_ss.at[j], sw_rs.at[j], to))
        switches[-1].start()
    step(0, 1)
    step(1, 1)
    step(2, 1)
    step(3, 1)
    step(1, 2)
    step(3, 2)
    step(0, 2)
    step(2, 2)
    step(1, 3)
    step(3, 3)

    for c in switches:
        c.wait()
    for c in pairs:
        c.wait_send()
    for o in range(3):
        share(o).wait_send()
    for i, part in enumerate(PARTS):
        for stage in range(4 if part.order == "y" else 3):
            for c in copies(i, stage):
                c.wait_send()

    @pl.when(sp < 7)
    def _():
        halo.wait_send()

    @pl.when(sp > 0)
    def _():
        slope_ct.wait_send()
        slope_part.wait_send()


def deliver(*refs):
    ins, outs, sem = refs[:3], refs[3:6], refs[6]
    moves = [pltpu.make_async_copy(a, b, sem.at[i]) for i, (a, b) in enumerate(zip(ins, outs))]
    for move in moves:
        move.start()
    for move in moves:
        move.wait()


RESULTS = (((32, 4096), BF), ((4, 1024, 128), BF), ((216, 256), F32))


def body(volume, weights, cotangent):
    count = 16 * 16 * 16 * 16
    vmem = pltpu.VMEM
    dma = pltpu.SemaphoreType.DMA
    whole = pl.BlockSpec(memory_space=pltpu.VMEM)
    far = pl.BlockSpec(memory_space=pltpu.HBM)
    results = pl.pallas_call(
        functools.partial(kernel, 1.0 / count**0.5),
        out_shape=tuple(pltpu.VMEM(shape, dtype) for shape, dtype in RESULTS),
        in_specs=[far] * 3,
        out_specs=(whole, whole, whole),
        scratch_shapes=[
            vmem((4, 1024, 128), BF),
            vmem((3456, 256), BF),
            vmem((512, 256), BF),
            vmem((1040, 128), F32),
            vmem((4, 256, 1152), BF),
            vmem((2, 4, 576, 256), BF),
            vmem((4, 576, 256), BF),
            vmem((3, 256, 256), BF),
            vmem((3, 256, 256), BF),
            vmem((3, 256, 256), BF),
            vmem((256, 256), BF),
            vmem((256, 256), BF),
            vmem((256, 256), BF),
            vmem((256, 256), BF),
            vmem((256, 256), BF),
            vmem((256, 512), BF),
            vmem((16, 64, 128), F32),
            dma((8,)),
            dma((7,)),
            dma((7,)),
            dma((3,)),
            dma((3,)),
            dma((7,)),
            dma((7,)),
            dma((SUMS,)),
            dma((SUMS,)),
            pltpu.SemaphoreType.REGULAR,
            *[shape for part in PARTS for shape in part.scratch()],
        ],
        compiler_params=pltpu.CompilerParams(
            collective_id=0, has_side_effects=True, vmem_limit_bytes=40 * 2**20
        ),
        name="conv_step",
    )(
        *(
            pltpu.with_memory_space_constraint(value, pltpu.HBM)
            for value in (
                volume.reshape(4, 1024, 128),
                weights.reshape(3456, 256),
                cotangent.reshape(512, 256),
            )
        )
    )
    switched, volume_grad, kernel_grad = pl.pallas_call(
        deliver,
        out_shape=tuple(jax.ShapeDtypeStruct(shape, dtype) for shape, dtype in RESULTS),
        in_specs=[whole] * 3,
        out_specs=[far] * 3,
        scratch_shapes=[dma((3,))],
        compiler_params=pltpu.CompilerParams(vmem_limit_bytes=8 * 2**20),
        name="deliver",
    )(*results)
    return (
        switched[None],
        volume_grad.reshape(1, 4, 32, 32, 128),
        kernel_grad.reshape(3, 3, 3, 8, 256),
    )


def solution(mesh):
    in_specs = (P("dp", "space", None, None, None), P(), P("dp", "space", None, None, None))
    out_specs = (
        P("dp", "space", None),
        P("dp", "space", None, None, None),
        P(None, None, None, "dp", None),
    )
    return jax.shard_map(body, mesh=mesh, in_specs=in_specs, out_specs=out_specs, check_vma=False)
```

```python
import functools

import jax
import jax.numpy as jnp
from jax import lax
from jax.experimental import pallas as pl
from jax.experimental.pallas import tpu as pltpu
from jax.sharding import PartitionSpec as P

MESH = pl.DeviceIdType.MESH
BF, F32 = jnp.bfloat16, jnp.float32
NT = (((1,), (1,)), ((), ()))
TAPS = 9
PAIRS = {0: ((1, 1), (3, 2)), 1: ((0, 0), (2, 1)), 2: ((1, 0), (3, 1))}
REACH = {0: ((0, 1),), 1: ((0, 2), (1, 0)), 2: ((1, 1),), 3: ((1, 2), (2, 0))}


def nt(a, b):
    return lax.dot_general(a, b, NT, preferred_element_type=F32)


def mm(a, b):
    return jnp.dot(a, b, preferred_element_type=F32)


class Part:
    def __init__(self, kd, low, count, order):
        self.kd, self.low, self.count, self.order = kd, low, count, order
        if order == "z":
            self.axes, self.held, self.starts = "zyx", count, (0,)
            self.sizes = ((4, 2 * count), (2, count), (1, count))
        else:
            self.axes, self.held = "yzx", (count + 1) // 2
            self.starts = (0, count - self.held)
            self.sizes = ((4, 4 * self.held), (4, self.held), (1, self.held))
        self.copies = (3, 3, 3 if order == "z" else 7)

    def scratch(self):
        shapes = []
        for (blocks, tiles), copies in zip(self.sizes, self.copies):
            shapes.append(pltpu.VMEM((blocks, tiles, 16, 128), F32))
            shapes.append(pltpu.VMEM((blocks, tiles, 16, 128), BF))
            shapes.append(pltpu.VMEM((copies, tiles, 16, 128), BF))
        return shapes


PARTS = (Part(1, 0, 9, "z"), Part(2, 0, 9, "y"), Part(0, 0, 5, "z"), Part(0, 5, 4, "z"))
ORDER = (
    (0, 0), (1, 0), (2, 0), (3, 0), (0, 1), (1, 1), (2, 1), (3, 1), (0, 2), (2, 2), (3, 2), (1, 2),
)
SUMS = sum(sum(part.copies) for part in PARTS)


def kernel(scale, vol_hbm, w_hbm, ct_hbm, sw_ref, vg_ref, kg_ref, *rest):
    (
        vol, w, ct, spread, taps, tt, ttr, gp, gps, gpr, hs, hr, ps, pr, cr, swb, crossed, fine, vg,
        in_sem, out_sem, pair_ss, pair_rs, edge_ss, edge_rs, sw_ss, sw_rs, sum_ss, sum_rs, ready,
    ) = rest[:30]
    rest, room, number = list(rest[30:]), {}, {}
    for i, part in enumerate(PARTS):
        count = len(part.scratch())
        room[i], rest = rest[:count], rest[count:]
        number[i] = sum(sum(p.copies) for p in PARTS[:i])

    dp, sp = lax.axis_index("dp"), lax.axis_index("space")
    core, z, y, x = dp % 2, (dp // 2) % 4, (sp // 4) * 2 + dp // 8, sp % 4
    y_hi = sp // 4

    def chip(x, y, z, core):
        return ((y % 2) * 8 + z * 2 + core, (y // 2) * 4 + x)

    partner = chip(x, y, z, 1 - core)
    along = {
        "z": [chip(x, y, (z + j) % 4, core) for j in (1, 2, 3)],
        "y": [chip(x, (y + j) % 4, z, core) for j in (1, 2, 3)],
        "x": [chip((x + j) % 4, y, z, core) for j in (1, 2, 3)],
    }
    slabs = [(dp, (sp + j) % 8) for j in range(1, 8)]
    above, below = (dp, (sp + 1) % 8), (dp, (sp + 7) % 8)

    def remote(src, dst, ss, rs, to):
        return pltpu.make_async_remote_copy(
            src_ref=src, dst_ref=dst, send_sem=ss, recv_sem=rs, device_id=to, device_id_type=MESH
        )

    def signal(sem, to):
        pl.semaphore_signal(sem, inc=1, device_id=to, device_id_type=MESH)

    loads = {}
    for i, p in enumerate((3, 0, 1, 2)):
        loads["v", p] = pltpu.make_async_copy(vol_hbm.at[p], vol.at[p], in_sem.at[i])
    for kd in range(3):
        rows = pl.ds(kd * 1152, 1152)
        loads["w", kd] = pltpu.make_async_copy(w_hbm.at[rows], w.at[rows], in_sem.at[4 + kd])
    loads["c"] = pltpu.make_async_copy(ct_hbm, ct, in_sem.at[7])
    for which in (("v", 3), ("w", 0), ("v", 0), ("v", 1), ("w", 1), ("w", 2), ("v", 2), "c"):
        loads[which].start()

    barrier = pltpu.get_barrier_semaphore()
    near = [along[axis][j] for axis in "xyz" for j in (0, 2)]
    for peer in [partner, *near]:
        signal(barrier, peer)

    @pl.when(sp == 3)
    def _():
        signal(barrier, above)

    @pl.when(sp == 4)
    def _():
        signal(barrier, below)

    def edge(condition, ref):
        @pl.when(condition)
        def _():
            ref[...] = jnp.zeros(ref.shape, ref.dtype)

    edge(sp == 7, gp.at[2])
    edge(sp == 0, hr)

    first_column = lax.broadcasted_iota(jnp.int32, (512, 128), 0) % 16 == 0
    last_column = lax.broadcasted_iota(jnp.int32, (256, 256), 0) % 16 == 15

    def unfold(p):
        loads["v", p].wait()
        spread[pl.ds(8, 1024)] = vol[p].astype(F32)
        even = spread[pl.ds(8, 512, stride=2)].astype(BF)
        odd = spread[pl.ds(9, 512, stride=2)].astype(BF)
        left = jnp.where(first_column, 0.0, spread[pl.ds(7, 512, stride=2)]).astype(BF)
        for kw, source in enumerate((left, even, odd)):
            rows = source.reshape(16, 32, 128)
            upper, lower = rows[:, :16], rows[:, 16:]
            before = jnp.concatenate([jnp.zeros((1, 16, 128), BF), lower[:-1]], axis=0)
            for kh, block in enumerate((before, upper, lower)):
                at = (kh * 3 + kw) * 128
                taps[p, :, at : at + 128] = block.reshape(256, 128)

    row = lax.broadcasted_iota(jnp.int32, (128, 128), 0)
    column = lax.broadcasted_iota(jnp.int32, (128, 128), 1)
    channel = (((row % 64) // 8) * 2 + row // 64) * 8 + row % 8
    sort = (column == channel).astype(F32).astype(BF)
    pairs = []

    def turn(p):
        for t in range(TAPS):
            turned = nt(sort, taps[p, :, t * 128 : (t + 1) * 128]).astype(BF)
            tt[0, p, t * 64 : (t + 1) * 64] = turned[:64]
            tt[1, p, t * 64 : (t + 1) * 64] = turned[64:]
        pairs.append(remote(tt.at[1 - core, p], ttr.at[p], pair_ss.at[p], pair_rs.at[p], partner))
        pairs[-1].start()

    er = lax.broadcasted_iota(jnp.int32, (256, 256), 0)
    ec = lax.broadcasted_iota(jnp.int32, (256, 256), 1)
    unit = (er == ec).astype(F32).astype(BF)

    def share(o):
        return remote(gp.at[o], gpr.at[o], pair_ss.at[4 + o], pair_rs.at[4 + o], partner)

    def to_right(o):
        value = gp[o].astype(F32)
        gps[o] = jnp.where(last_column, 0.0, pltpu.roll(value, 255, 0)).astype(BF)

    def slope_of(v):
        s = jax.nn.sigmoid(v)
        return s, s * (1.0 + v * (1.0 - s))

    def finish(o, v):
        s, slope = slope_of(v)
        gp[o] = (ct[pl.ds(o * 256, 256)].astype(F32) * slope).astype(BF)
        swb[o] = nt(unit, (v * s).astype(BF)).astype(BF)

    planes = []

    def grad_plane(p):
        for half, moves in ((0, ((1, 0),)), (1, ((2, 0), (0, 1)))):
            lhs, lhs_right, rhs, rhs_right = [], [], [], []
            for o, kd in REACH[p]:
                for kh, down in moves:
                    for source, out in ((gp, lhs), (gps, lhs_right)):
                        value = source[o]
                        if down:
                            value = jnp.concatenate([value[16:], jnp.zeros((16, 256), BF)], axis=0)
                        out.append(value)
                    at = (kd * 9 + kh * 3) * 128
                    rhs_right.append(w[at : at + 128])
                    rhs.append(w[at + 128 : at + 384])
            both = nt(jnp.concatenate(lhs, axis=1), jnp.concatenate(rhs, axis=1))
            more = nt(jnp.concatenate(lhs_right, axis=1), jnp.concatenate(rhs_right, axis=1))
            fine[:, pl.ds(half * 32, 16, stride=2), :] = both[:, :128].reshape(16, 16, 128)
            fine[:, pl.ds(half * 32 + 1, 16, stride=2), :] = (both[:, 128:] + more).reshape(16, 16, 128)
        vg[p] = fine[...].reshape(1024, 128).astype(BF)
        planes.append(pltpu.make_async_copy(vg.at[p], vg_ref.at[p], out_sem.at[p]))
        planes[-1].start()

    def own_part(kd):
        (a, oa), (b, ob) = PAIRS[kd]
        lhs = jnp.concatenate([tt[core, a], tt[core, b]], axis=1)
        return mm(lhs, jnp.concatenate([gp[oa], gp[ob]], axis=0))

    def pair_part(kd):
        (a, oa), (b, ob) = PAIRS[kd]
        lhs = jnp.concatenate([ttr[a], ttr[b]], axis=1)
        return mm(lhs, jnp.concatenate([gpr[oa], gpr[ob]], axis=0))

    place = {"x": x, "y": y, "z": z}
    across = [chip((x + j) % 4, (y + 2) % 4, z, core) for j in range(4)]

    def copies(i, stage):
        part, refs, out = PARTS[i], room[i], []
        axis, blocks = part.axes[stage], part.sizes[stage][0]
        peers = along[axis] + (across if part.copies[stage] == 7 else [])
        for j, to in enumerate(peers):
            at = number[i] + stage * 3 + j
            src = refs[3 * stage + 1].at[(place[axis] + j + 1) % blocks]
            out.append(remote(src, refs[3 * stage + 2].at[j], sum_ss.at[at], sum_rs.at[at], to))
        return out

    def send(i, stage):
        for c in reversed(copies(i, stage)):
            c.start()

    def put(i, total):
        part, refs = PARTS[i], room[i]
        for t in range(part.count):
            for group in range(8):
                at = (part.low + t) * 64 + group * 8
                tile = jnp.concatenate([total[at : at + 8, :128], total[at : at + 8, 128:]], axis=0)
                half = tile.astype(BF)
                y_lo, to_z = group // 4, group % 4
                for n, start in enumerate(part.starts):
                    k = t - start
                    if not 0 <= k < part.held:
                        continue
                    if part.order == "z":
                        block, where = to_z, y_lo * part.held + k
                    else:
                        block, where = n * 2 + y_lo, to_z * part.held + k
                    refs[0][block, where] = tile
                    refs[1][block, where] = half
        send(i, 0)

    def write(part, start, value):
        value = value * scale
        for t in range(part.held):
            at = pl.multiple_of((part.kd * 9 + part.low + start + t) * 8, 8)
            kg_ref[pl.ds(at, 8), 0:128] = value[t, 0:8]
            kg_ref[pl.ds(at, 8), 128:256] = value[t, 8:16]

    def step(i, stage):
        part, refs = PARTS[i], room[i]
        for c in copies(i, stage):
            c.wait_recv()
        own, _, got = refs[3 * stage : 3 * stage + 3]
        total = own[place[part.axes[stage]] % part.sizes[stage][0]]
        for j in range(3):
            total = total + got[j].astype(F32)
        if stage < 2:
            total = total.reshape(*part.sizes[stage + 1], 16, 128)
            refs[3 * stage + 3][...] = total
            refs[3 * stage + 4][...] = total.astype(BF)
            send(i, stage + 1)
        elif part.order == "z":
            write(part, 0, total)
        else:
            other = got[3].astype(F32)
            for j in (4, 5, 6):
                other = other + got[j].astype(F32)
            write(part, y_hi * part.starts[1], total)
            write(part, (1 - y_hi) * part.starts[1], other)

    other_row = along["y"][1]
    switches, locals_, crossings = [], [], []

    def cells(slab, o):
        return pl.ds(pl.multiple_of(slab * 512 + o * 256, 256), 256)

    def hand_out(at, rows_of, slab, o):
        for j in range(4):
            rows = pl.ds(pl.multiple_of((x + j) % 4 * 32, 32), 32)
            src, dst = rows_of.at[rows], sw_ref.at[:, cells(slab, o)]
            if j == 0:
                locals_.append(pltpu.make_async_copy(src, dst, out_sem.at[4 + at // 3]))
                locals_[-1].start()
            else:
                k = at + j - 1
                switches.append(remote(src, dst, sw_ss.at[k], sw_rs.at[k], along["x"][j - 1]))
                switches[-1].start()

    def switch(o):
        rows = pl.ds(pl.multiple_of((1 - y_hi) * 128, 128), 128)
        crossings.append(remote(swb.at[o, rows], crossed.at[o], sw_ss.at[12 + o], sw_rs.at[12 + o], other_row))
        crossings[-1].start()
        rows = pl.ds(pl.multiple_of(y_hi * 128, 128), 128)
        hand_out(o * 3, swb.at[o, rows], sp, o)

    def switch_on():
        for o, crossing in zip((1, 0), crossings):
            crossing.wait_recv()
            hand_out(6 + o * 3, crossed.at[o], (1 - y_hi) * 4 + x, o)

    spread[0:8] = jnp.zeros((8, 128), F32)
    unfold(3)
    loads["w", 0].wait()
    hs[...] = mm(taps[3], w[0:1152]).astype(BF)

    pl.semaphore_wait(barrier, 7 + jnp.where((sp == 3) | (sp == 4), 1, 0))
    halo = remote(hs, hr, edge_ss.at[0], edge_rs.at[0], above)
    slope_part = remote(ps, pr, edge_ss.at[1], edge_rs.at[1], below)
    slope_ct = remote(ct_hbm.at[pl.ds(0, 256)], cr, edge_ss.at[2], edge_rs.at[2], below)

    @pl.when(sp < 7)
    def _():
        halo.start()

    @pl.when(sp > 0)
    def _():
        slope_ct.start()

    for peer in near:
        signal(ready, peer)

    unfold(0)
    unfold(1)
    loads["w", 1].wait()
    loads["w", 2].wait()
    pre0 = mm(taps[0], w[1152:2304]) + mm(taps[1], w[2304:3456])
    ps[...] = pre0.astype(BF)

    @pl.when(sp > 0)
    def _():
        slope_part.start()

    turn(3)
    turn(1)
    turn(0)
    unfold(2)
    turn(2)
    pre1 = mm(taps[1], w[0:1152]) + mm(taps[2], w[1152:2304]) + mm(taps[3], w[2304:3456])
    loads["c"].wait()
    finish(1, pre1)
    share(1).start()
    pl.semaphore_wait(ready, len(near))
    switch(1)
    to_right(1)

    @pl.when(sp > 0)
    def _():
        halo.wait_recv()

    finish(0, pre0 + hr[...].astype(F32))
    share(0).start()
    switch(0)

    part1, part2 = own_part(1), own_part(2)
    for c in pairs:
        c.wait_recv()
    share(1).wait_recv()
    share(0).wait_recv()
    put(0, part1 + pair_part(1))
    put(1, part2 + pair_part(2))

    @pl.when(sp < 7)
    def _():
        slope_ct.wait_recv()
        slope_part.wait_recv()
        _, slope = slope_of(pr[...].astype(F32) + hs[...].astype(F32))
        gp[2] = (cr[...].astype(F32) * slope).astype(BF)

    share(2).start()
    part0 = own_part(0)
    grad_plane(2)
    share(2).wait_recv()
    total0 = part0 + pair_part(0)
    put(2, total0)
    put(3, total0)
    to_right(0)
    to_right(2)
    switch_on()
    for p in (0, 1, 3):
        grad_plane(p)

    for i, stage in ORDER:
        step(i, stage)

    for c in planes + locals_:
        c.wait()
    for c in crossings:
        c.wait_send()
    for c in switches:
        c.wait()
    for c in pairs:
        c.wait_send()
    for o in range(3):
        share(o).wait_send()
    for i, part in enumerate(PARTS):
        for stage in range(3):
            for c in copies(i, stage):
                c.wait_send()

    @pl.when(sp < 7)
    def _():
        halo.wait_send()

    @pl.when(sp > 0)
    def _():
        slope_ct.wait_send()
        slope_part.wait_send()


def deliver(*refs):
    ins, outs, sem = refs[:3], refs[3:6], refs[6]
    moves = [pltpu.make_async_copy(a, b, sem.at[i]) for i, (a, b) in enumerate(zip(ins, outs))]
    for move in moves:
        move.start()
    for move in moves:
        move.wait()


RESULTS = (((32, 4096), BF), ((4, 1024, 128), BF), ((216, 256), F32))


def body(volume, weights, cotangent):
    count = 16 * 16 * 16 * 16
    vmem = pltpu.VMEM
    dma = pltpu.SemaphoreType.DMA
    whole = pl.BlockSpec(memory_space=pltpu.VMEM)
    far = pl.BlockSpec(memory_space=pltpu.HBM)
    anywhere = pl.BlockSpec(memory_space=pl.ANY)
    results = pl.pallas_call(
        functools.partial(kernel, 1.0 / count**0.5),
        out_shape=tuple(pltpu.VMEM(shape, dtype) for shape, dtype in RESULTS),
        in_specs=[far] * 3,
        out_specs=(anywhere, anywhere, whole),
        scratch_shapes=[
            vmem((4, 1024, 128), BF),
            vmem((3456, 256), BF),
            vmem((512, 256), BF),
            vmem((1040, 128), F32),
            vmem((4, 256, 1152), BF),
            vmem((2, 4, 576, 256), BF),
            vmem((4, 576, 256), BF),
            vmem((3, 256, 256), BF),
            vmem((3, 256, 256), BF),
            vmem((3, 256, 256), BF),
            vmem((256, 256), BF),
            vmem((256, 256), BF),
            vmem((256, 256), BF),
            vmem((256, 256), BF),
            vmem((256, 256), BF),
            vmem((2, 256, 256), BF),
            vmem((2, 128, 256), BF),
            vmem((16, 64, 128), F32),
            vmem((4, 1024, 128), BF),
            dma((8,)),
            dma((8,)),
            dma((7,)),
            dma((7,)),
            dma((3,)),
            dma((3,)),
            dma((14,)),
            dma((14,)),
            dma((SUMS,)),
            dma((SUMS,)),
            pltpu.SemaphoreType.REGULAR,
            *[shape for part in PARTS for shape in part.scratch()],
        ],
        compiler_params=pltpu.CompilerParams(
            collective_id=0, has_side_effects=True, vmem_limit_bytes=40 * 2**20
        ),
        name="conv_step",
    )(
        *(
            pltpu.with_memory_space_constraint(value, pltpu.HBM)
            for value in (
                volume.reshape(4, 1024, 128),
                weights.reshape(3456, 256),
                cotangent.reshape(512, 256),
            )
        )
    )
    switched, volume_grad, kernel_grad = pl.pallas_call(
        deliver,
        out_shape=tuple(jax.ShapeDtypeStruct(shape, dtype) for shape, dtype in RESULTS),
        in_specs=[anywhere] * 3,
        out_specs=[far] * 3,
        scratch_shapes=[dma((3,))],
        compiler_params=pltpu.CompilerParams(vmem_limit_bytes=8 * 2**20),
        name="deliver",
    )(*results)
    return (
        switched[None],
        volume_grad.reshape(1, 4, 32, 32, 128),
        kernel_grad.reshape(3, 3, 3, 8, 256),
    )


def solution(mesh):
    in_specs = (P("dp", "space", None, None, None), P(), P("dp", "space", None, None, None))
    out_specs = (
        P("dp", "space", None),
        P("dp", "space", None, None, None),
        P(None, None, None, "dp", None),
    )
    return jax.shard_map(body, mesh=mesh, in_specs=in_specs, out_specs=out_specs, check_vma=False)
```

```python
import functools

import jax
import jax.numpy as jnp
from jax import lax
from jax.experimental import pallas as pl
from jax.experimental.pallas import tpu as pltpu
from jax.sharding import PartitionSpec as P

MESH = pl.DeviceIdType.MESH
BF, F32 = jnp.bfloat16, jnp.float32
NT = (((1,), (1,)), ((), ()))
TAPS = 9
PAIRS = {0: ((1, 1), (3, 2)), 1: ((0, 0), (2, 1)), 2: ((1, 0), (3, 1))}
REACH = {0: ((0, 1),), 1: ((0, 2), (1, 0)), 2: ((1, 1),), 3: ((1, 2), (2, 0))}


def nt(a, b):
    return lax.dot_general(a, b, NT, preferred_element_type=F32)


def mm(a, b):
    return jnp.dot(a, b, preferred_element_type=F32)


class Part:
    def __init__(self, kd, low, count, order):
        self.kd, self.low, self.count, self.order = kd, low, count, order
        self.axes, self.first = order, order[0]
        self.held, self.starts = count, (0,)
        self.copies, self.gathered = (3, 3, 3), False
        if order == "zyx":
            self.sizes = ((4, 2 * count), (2, count), (1, count))
        elif order == "zxy":
            self.sizes = ((4, 2 * count), (1, 2 * count), (2, count))
        elif order[0] == "y":
            self.held = (count + 1) // 2
            self.starts = (0, count - self.held)
            self.sizes = ((4, 4 * self.held), (4, self.held), (1, self.held))
            self.copies = (3, 3, 7 if order == "yzx" else 3)
            self.gathered = order == "yzxy"
        else:
            self.held = (count + 3) // 4
            self.starts = tuple((count - self.held) * i // 3 for i in range(4))
            self.sizes = ((4, 8 * self.held), (4, 2 * self.held), (2, self.held))
            self.gathered = True

    def scratch(self):
        shapes = []
        for (blocks, tiles), copies in zip(self.sizes, self.copies):
            shapes.append(pltpu.VMEM((blocks, tiles, 16, 128), F32))
            shapes.append(pltpu.VMEM((blocks, tiles, 16, 128), BF))
            shapes.append(pltpu.VMEM((copies, tiles, 16, 128), BF))
        if self.gathered:
            shapes.append(pltpu.VMEM((self.held, 16, 128), F32))
            shapes.append(pltpu.VMEM((3 if self.first == "x" else 1, self.held, 16, 128), F32))
        return shapes


PARTS = (Part(1, 0, 9, "zyx"), Part(2, 0, 9, "yzx"), Part(0, 0, 5, "zyx"), Part(0, 5, 4, "yzx"),)
ORDER = ((0, 0), (1, 0), (2, 0), (3, 0), (0, 1), (1, 1), (2, 1), (3, 1), (0, 2), (2, 2), (3, 2), (1, 2))
DURING = {(0, 0): 0, (2, 0): 1, (0, 2): 3}
SUMS = 4 * len(PARTS)


def kernel(scale, vol_hbm, w_hbm, ct_hbm, sw_ref, vg_ref, kg_ref, *rest):
    (
        vol, w, ct, spread, taps, tt, ttr, gp, gps, gpr, hs, hr, ps, pr, cr, swb, crossed, fine, vg, own,
        in_sem, out_sem, pair_ss, pair_rs, edge_ss, edge_rs, sw_ss, sw_rs, sum_ss, sum_rs, ready,
    ) = rest[:31]
    rest, room = list(rest[31:]), {}
    for i, part in enumerate(PARTS):
        count = len(part.scratch())
        room[i], rest = rest[:count], rest[count:]

    dp, sp = lax.axis_index("dp"), lax.axis_index("space")
    core, z, y, x = dp % 2, (dp // 2) % 4, (sp // 4) * 2 + dp // 8, sp % 4
    y_hi = sp // 4

    def chip(x, y, z, core):
        return ((y % 2) * 8 + z * 2 + core, (y // 2) * 4 + x)

    partner = chip(x, y, z, 1 - core)
    along = {
        "z": [chip(x, y, (z + j) % 4, core) for j in (1, 2, 3)],
        "y": [chip(x, (y + j) % 4, z, core) for j in (1, 2, 3)],
        "x": [chip((x + j) % 4, y, z, core) for j in (1, 2, 3)],
    }
    slabs = [(dp, (sp + j) % 8) for j in range(1, 8)]
    above, below = (dp, (sp + 1) % 8), (dp, (sp + 7) % 8)

    def remote(src, dst, ss, rs, to):
        return pltpu.make_async_remote_copy(
            src_ref=src, dst_ref=dst, send_sem=ss, recv_sem=rs, device_id=to, device_id_type=MESH
        )

    def signal(sem, to):
        pl.semaphore_signal(sem, inc=1, device_id=to, device_id_type=MESH)

    def landed(ref, sem):
        pltpu.make_async_copy(ref, ref, sem).wait()

    barrier = pltpu.get_barrier_semaphore()
    near = [along[axis][j] for axis in "xyz" for j in (0, 2)]
    for peer in [partner, *near]:
        signal(barrier, peer)

    @pl.when(sp == 3)
    def _():
        signal(barrier, above)

    @pl.when(sp == 4)
    def _():
        signal(barrier, below)

    loads = {}
    for i, p in enumerate((3, 0, 1, 2)):
        loads["v", p] = pltpu.make_async_copy(vol_hbm.at[p], vol.at[p], in_sem.at[i])
    for kd in range(3):
        rows = pl.ds(kd * 1152, 1152)
        loads["w", kd] = pltpu.make_async_copy(w_hbm.at[rows], w.at[rows], in_sem.at[4 + kd])
    loads["c"] = pltpu.make_async_copy(ct_hbm, ct, in_sem.at[7])
    for which in (("v", 3), ("w", 0), ("v", 0), ("v", 1), ("w", 1), ("w", 2), ("v", 2), "c"):
        loads[which].start()

    def edge(condition, ref):
        @pl.when(condition)
        def _():
            ref[...] = jnp.zeros(ref.shape, ref.dtype)

    edge(sp == 7, gp.at[2])
    edge(sp == 0, hr)

    first_column = lax.broadcasted_iota(jnp.int32, (512, 128), 0) % 16 == 0
    last_column = lax.broadcasted_iota(jnp.int32, (256, 256), 0) % 16 == 15

    def unfold(p):
        loads["v", p].wait()
        spread[pl.ds(8, 1024)] = vol[p].astype(F32)
        even = spread[pl.ds(8, 512, stride=2)].astype(BF)
        odd = spread[pl.ds(9, 512, stride=2)].astype(BF)
        left = jnp.where(first_column, 0.0, spread[pl.ds(7, 512, stride=2)]).astype(BF)
        for kw, source in enumerate((left, even, odd)):
            rows = source.reshape(16, 32, 128)
            upper, lower = rows[:, :16], rows[:, 16:]
            before = jnp.concatenate([jnp.zeros((1, 16, 128), BF), lower[:-1]], axis=0)
            for kh, block in enumerate((before, upper, lower)):
                at = (kh * 3 + kw) * 128
                taps[p, :, at : at + 128] = block.reshape(256, 128)

    row = lax.broadcasted_iota(jnp.int32, (128, 128), 0)
    column = lax.broadcasted_iota(jnp.int32, (128, 128), 1)
    channel = (((row % 64) // 8) * 2 + row // 64) * 8 + row % 8
    sort = (column == channel).astype(F32).astype(BF)

    def turn(p):
        for t in range(TAPS):
            turned = nt(sort, taps[p, :, t * 128 : (t + 1) * 128]).astype(BF)
            tt[0, p, t * 64 : (t + 1) * 64] = turned[:64]
            tt[1, p, t * 64 : (t + 1) * 64] = turned[64:]
        remote(tt.at[1 - core, p], ttr.at[p], pair_ss.at[3], pair_rs.at[3], partner).start()

    er = lax.broadcasted_iota(jnp.int32, (256, 256), 0)
    ec = lax.broadcasted_iota(jnp.int32, (256, 256), 1)
    unit = (er == ec).astype(F32).astype(BF)

    def share(o):
        return remote(gp.at[o], gpr.at[o], pair_ss.at[o], pair_rs.at[o], partner)

    def to_right(o):
        value = gp[o].astype(F32)
        gps[o] = jnp.where(last_column, 0.0, pltpu.roll(value, 255, 0)).astype(BF)

    def slope_of(v):
        s = jax.nn.sigmoid(v)
        return s, s * (1.0 + v * (1.0 - s))

    def finish(o, v):
        s, slope = slope_of(v)
        gp[o] = (ct[pl.ds(o * 256, 256)].astype(F32) * slope).astype(BF)
        swb[o] = nt(unit, (v * s).astype(BF)).astype(BF)

    def grad_plane(p):
        for half, moves in ((0, ((1, 0),)), (1, ((2, 0), (0, 1)))):
            lhs, lhs_right, rhs, rhs_right = [], [], [], []
            for o, kd in REACH[p]:
                for kh, down in moves:
                    for source, out in ((gp, lhs), (gps, lhs_right)):
                        value = source[o]
                        if down:
                            value = jnp.concatenate([value[16:], jnp.zeros((16, 256), BF)], axis=0)
                        out.append(value)
                    at = (kd * 9 + kh * 3) * 128
                    rhs_right.append(w[at : at + 128])
                    rhs.append(w[at + 128 : at + 384])
            both = nt(jnp.concatenate(lhs, axis=1), jnp.concatenate(rhs, axis=1))
            more = nt(jnp.concatenate(lhs_right, axis=1), jnp.concatenate(rhs_right, axis=1))
            fine[:, pl.ds(half * 32, 16, stride=2), :] = both[:, :128].reshape(16, 16, 128)
            fine[:, pl.ds(half * 32 + 1, 16, stride=2), :] = (both[:, 128:] + more).reshape(16, 16, 128)
        vg[p] = fine[...].reshape(1024, 128).astype(BF)
        pltpu.make_async_copy(vg.at[p], vg_ref.at[p], out_sem.at[0]).start()

    def own_part(kd):
        (a, oa), (b, ob) = PAIRS[kd]
        lhs = jnp.concatenate([tt[core, a], tt[core, b]], axis=1)
        own[kd] = mm(lhs, jnp.concatenate([gp[oa], gp[ob]], axis=0))

    def pair_part(kd):
        (a, oa), (b, ob) = PAIRS[kd]
        lhs = jnp.concatenate([ttr[a], ttr[b]], axis=1)
        return mm(lhs, jnp.concatenate([gpr[oa], gpr[ob]], axis=0))

    place = {"x": x, "y": y, "z": z}
    across = [chip((x + j) % 4, (y + 2) % 4, z, core) for j in range(4)]

    def copies(i, stage):
        part, refs, out = PARTS[i], room[i], []
        at = i * 4 + stage
        if stage == 3:
            return [
                remote(refs[9], refs[10].at[j], sum_ss.at[at], sum_rs.at[at], to)
                for j, to in enumerate(along["x"] if part.first == "x" else along["y"][1:2])
            ]
        axis, blocks = part.axes[stage], part.sizes[stage][0]
        peers = along[axis] + (across if part.copies[stage] == 7 else [])
        for j, to in enumerate(peers):
            src = refs[3 * stage + 1].at[(place[axis] + j + 1) % blocks]
            out.append(remote(src, refs[3 * stage + 2].at[j], sum_ss.at[at], sum_rs.at[at], to))
        return out

    def arrived(i, stage, sems):
        landed(room[i][10 if stage == 3 else 3 * stage + 2], sems.at[i * 4 + stage])

    def send(i, stage):
        for c in reversed(copies(i, stage)):
            c.start()

    def put(i, total):
        part, refs = PARTS[i], room[i]
        for t in range(part.count):
            for group in range(8):
                at = (part.low + t) * 64 + group * 8
                tile = jnp.concatenate([total[at : at + 8, :128], total[at : at + 8, 128:]], axis=0)
                half = tile.astype(BF)
                y_lo, to_z = group // 4, group % 4
                for n, start in enumerate(part.starts):
                    k = t - start
                    if not 0 <= k < part.held:
                        continue
                    if part.first == "z":
                        block, where = to_z, y_lo * part.held + k
                    elif part.first == "y":
                        block, where = n * 2 + y_lo, to_z * part.held + k
                    else:
                        block, where = n, (to_z * 2 + y_lo) * part.held + k
                    refs[0][block, where] = tile
                    refs[1][block, where] = half
        send(i, 0)

    def put_all(kd, total):
        for i, part in enumerate(PARTS):
            if part.kd == kd:
                put(i, total)

    def write(part, owner, value):
        stride = part.starts[1] if len(part.starts) > 1 else 0
        value = value * scale
        for t in range(part.held):
            at = pl.multiple_of((part.kd * 9 + part.low + owner * stride + t) * 8, 8)
            kg_ref[pl.ds(at, 8), 0:128] = value[t, 0:8]
            kg_ref[pl.ds(at, 8), 128:256] = value[t, 8:16]

    def step(i, stage):
        part, refs = PARTS[i], room[i]
        arrived(i, stage, sum_rs)
        if stage == 3:
            if part.first == "y":
                write(part, 1 - y_hi, refs[10][0])
            else:
                for j in range(3):
                    write(part, (x + 3 - j) % 4, refs[10][j])
            return
        kept, _, got = refs[3 * stage : 3 * stage + 3]
        total = kept[place[part.axes[stage]] % part.sizes[stage][0]]
        for j in range(3):
            total = total + got[j].astype(F32)
        if stage < 2:
            total = total.reshape(*part.sizes[stage + 1], 16, 128)
            refs[3 * stage + 3][...] = total
            refs[3 * stage + 4][...] = total.astype(BF)
            send(i, stage + 1)
            return
        if part.gathered:
            refs[9][...] = total
            send(i, 3)
        write(part, {"z": 0, "y": y_hi, "x": x}[part.first], total)
        if part.copies[2] == 7:
            other = got[3].astype(F32)
            for j in (4, 5, 6):
                other = other + got[j].astype(F32)
            write(part, 1 - y_hi, other)

    other_row = along["y"][1]
    crossings = []

    def cells(slab, o):
        return pl.ds(pl.multiple_of(slab * 512 + o * 256, 256), 256)

    def hand_out(rows_of, slab, o):
        for j in range(4):
            rows = pl.ds(pl.multiple_of((x + j) % 4 * 32, 32), 32)
            src, dst = rows_of.at[rows], sw_ref.at[:, cells(slab, o)]
            if j == 0:
                pltpu.make_async_copy(src, dst, out_sem.at[1]).start()
            else:
                remote(src, dst, sw_ss.at[2], sw_rs.at[2], along["x"][j - 1]).start()

    def switch(o):
        rows = pl.ds(pl.multiple_of((1 - y_hi) * 128, 128), 128)
        crossings.append(remote(swb.at[o, rows], crossed.at[o], sw_ss.at[o], sw_rs.at[o], other_row))
        crossings[-1].start()
        rows = pl.ds(pl.multiple_of(y_hi * 128, 128), 128)
        hand_out(swb.at[o, rows], sp, o)

    def switch_on():
        for o, crossing in zip((1, 0), crossings):
            crossing.wait_recv()
            hand_out(crossed.at[o], (1 - y_hi) * 4 + x, o)

    spread[0:8] = jnp.zeros((8, 128), F32)
    unfold(3)
    loads["w", 0].wait()
    hs[...] = mm(taps[3], w[0:1152]).astype(BF)

    pl.semaphore_wait(barrier, 7 + jnp.where((sp == 3) | (sp == 4), 1, 0))
    halo = remote(hs, hr, edge_ss.at[0], edge_rs.at[0], above)
    slope_part = remote(ps, pr, edge_ss.at[1], edge_rs.at[1], below)
    slope_ct = remote(ct_hbm.at[pl.ds(0, 256)], cr, edge_ss.at[2], edge_rs.at[2], below)

    @pl.when(sp < 7)
    def _():
        halo.start()

    @pl.when(sp > 0)
    def _():
        slope_ct.start()

    for peer in near:
        signal(ready, peer)

    unfold(0)
    unfold(1)
    loads["w", 1].wait()
    loads["w", 2].wait()
    pre0 = mm(taps[0], w[1152:2304]) + mm(taps[1], w[2304:3456])
    ps[...] = pre0.astype(BF)

    @pl.when(sp > 0)
    def _():
        slope_part.start()

    turn(3)
    turn(1)
    turn(0)
    unfold(2)
    turn(2)
    pre1 = mm(taps[1], w[0:1152]) + mm(taps[2], w[1152:2304]) + mm(taps[3], w[2304:3456])
    loads["c"].wait()
    finish(1, pre1)
    share(1).start()
    pl.semaphore_wait(ready, len(near))
    switch(1)
    to_right(1)

    @pl.when(sp > 0)
    def _():
        halo.wait_recv()

    finish(0, pre0 + hr[...].astype(F32))
    share(0).start()
    switch(0)

    own_part(1)
    own_part(2)
    landed(ttr, pair_rs.at[3])
    share(1).wait_recv()
    share(0).wait_recv()
    total1 = own[1] + pair_part(1)
    put_all(1, total1)
    total2 = own[2] + pair_part(2)
    put_all(2, total2)

    @pl.when(sp < 7)
    def _():
        slope_ct.wait_recv()
        slope_part.wait_recv()
        _, slope = slope_of(pr[...].astype(F32) + hs[...].astype(F32))
        gp[2] = (cr[...].astype(F32) * slope).astype(BF)

    share(2).start()
    own_part(0)
    grad_plane(2)
    share(2).wait_recv()
    total0 = own[0] + pair_part(0)
    put_all(0, total0)
    to_right(0)
    to_right(2)
    switch_on()
    for i, stage in ORDER:
        if (i, stage) in DURING:
            grad_plane(DURING[i, stage])
        step(i, stage)

    landed(vg, out_sem.at[0])
    landed(sw_ref.at[:, pl.ds(0, 1024)], out_sem.at[1])
    landed(sw_ref.at[:, pl.ds(0, 3072)], sw_rs.at[2])
    landed(sw_ref.at[:, pl.ds(0, 3072)], sw_ss.at[2])
    for c in crossings:
        c.wait_send()
    landed(ttr, pair_ss.at[3])
    for o in range(3):
        share(o).wait_send()
    for i, stage in ORDER:
        arrived(i, stage, sum_ss)

    @pl.when(sp < 7)
    def _():
        halo.wait_send()

    @pl.when(sp > 0)
    def _():
        slope_ct.wait_send()
        slope_part.wait_send()


def deliver(sw_in, vg_in, kg_in, sw_out, vg_out, kg_out, sem):
    moves = [(kg_in, kg_out), (sw_in, sw_out)]
    moves += [(vg_in.at[p], vg_out.at[p]) for p in range(4)]
    moves = [pltpu.make_async_copy(a, b, sem.at[i]) for i, (a, b) in enumerate(moves)]
    for move in moves:
        move.start()
    for move in moves:
        move.wait()


RESULTS = (((32, 4096), BF), ((4, 1024, 128), BF), ((216, 256), F32))


def body(volume, weights, cotangent):
    count = 16 * 16 * 16 * 16
    vmem = pltpu.VMEM
    dma = pltpu.SemaphoreType.DMA
    whole = pl.BlockSpec(memory_space=pltpu.VMEM)
    far = pl.BlockSpec(memory_space=pltpu.HBM)
    anywhere = pl.BlockSpec(memory_space=pl.ANY)
    results = pl.pallas_call(
        functools.partial(kernel, 1.0 / count**0.5),
        out_shape=tuple(pltpu.VMEM(shape, dtype) for shape, dtype in RESULTS),
        in_specs=[far] * 3,
        out_specs=(anywhere, anywhere, whole),
        scratch_shapes=[
            vmem((4, 1024, 128), BF),
            vmem((3456, 256), BF),
            vmem((512, 256), BF),
            vmem((1040, 128), F32),
            vmem((4, 256, 1152), BF),
            vmem((2, 4, 576, 256), BF),
            vmem((4, 576, 256), BF),
            vmem((3, 256, 256), BF),
            vmem((3, 256, 256), BF),
            vmem((3, 256, 256), BF),
            vmem((256, 256), BF),
            vmem((256, 256), BF),
            vmem((256, 256), BF),
            vmem((256, 256), BF),
            vmem((256, 256), BF),
            vmem((2, 256, 256), BF),
            vmem((2, 128, 256), BF),
            vmem((16, 64, 128), F32),
            vmem((4, 1024, 128), BF),
            vmem((3, 576, 256), F32),
            dma((8,)),
            dma((2,)),
            dma((4,)),
            dma((4,)),
            dma((3,)),
            dma((3,)),
            dma((3,)),
            dma((3,)),
            dma((SUMS,)),
            dma((SUMS,)),
            pltpu.SemaphoreType.REGULAR,
            *[shape for part in PARTS for shape in part.scratch()],
        ],
        compiler_params=pltpu.CompilerParams(
            collective_id=0, has_side_effects=True, vmem_limit_bytes=40 * 2**20
        ),
        name="conv_step",
    )(
        *(
            pltpu.with_memory_space_constraint(value, pltpu.HBM)
            for value in (
                volume.reshape(4, 1024, 128),
                weights.reshape(3456, 256),
                cotangent.reshape(512, 256),
            )
        )
    )
    switched, volume_grad, kernel_grad = pl.pallas_call(
        deliver,
        out_shape=tuple(jax.ShapeDtypeStruct(shape, dtype) for shape, dtype in RESULTS),
        in_specs=[anywhere] * 3,
        out_specs=[far] * 3,
        scratch_shapes=[dma((6,))],
        compiler_params=pltpu.CompilerParams(vmem_limit_bytes=8 * 2**20),
        name="deliver",
    )(*results)
    return (
        switched[None],
        volume_grad.reshape(1, 4, 32, 32, 128),
        kernel_grad.reshape(3, 3, 3, 8, 256),
    )


def solution(mesh):
    in_specs = (P("dp", "space", None, None, None), P(), P("dp", "space", None, None, None))
    out_specs = (
        P("dp", "space", None),
        P("dp", "space", None, None, None),
        P(None, None, None, "dp", None),
    )
    return jax.shard_map(body, mesh=mesh, in_specs=in_specs, out_specs=out_specs, check_vma=False)
```

```python
import functools

import jax
import jax.numpy as jnp
from jax import lax
from jax.experimental import pallas as pl
from jax.experimental.pallas import tpu as pltpu
from jax.sharding import PartitionSpec as P

MESH = pl.DeviceIdType.MESH
BF, F32 = jnp.bfloat16, jnp.float32
NT = (((1,), (1,)), ((), ()))
TAPS = 9
PAIRS = {0: ((1, 1), (3, 2)), 1: ((0, 0), (2, 1)), 2: ((1, 0), (3, 1))}
REACH = {0: ((0, 1),), 1: ((0, 2), (1, 0)), 2: ((1, 1),), 3: ((1, 2), (2, 0))}


def nt(a, b):
    return lax.dot_general(a, b, NT, preferred_element_type=F32)


def mm(a, b):
    return jnp.dot(a, b, preferred_element_type=F32)


class Part:
    def __init__(self, kd, low, count, order):
        self.kd, self.low, self.count, self.order = kd, low, count, order
        self.axes, self.first = order, order[0]
        self.held, self.starts = count, (0,)
        self.copies, self.gathered = (3, 3, 3), False
        if order == "zyx":
            self.sizes = ((4, 2 * count), (2, count), (1, count))
        elif order == "zxy":
            self.sizes = ((4, 2 * count), (1, 2 * count), (2, count))
        elif order[0] == "y":
            self.held = (count + 1) // 2
            self.starts = (0, count - self.held)
            self.sizes = ((4, 4 * self.held), (4, self.held), (1, self.held))
            self.copies = (3, 3, 7 if order == "yzx" else 3)
            self.gathered = order == "yzxy"
        else:
            self.held = (count + 3) // 4
            self.starts = tuple((count - self.held) * i // 3 for i in range(4))
            self.sizes = ((4, 8 * self.held), (4, 2 * self.held), (2, self.held))
            self.gathered = True

    def scratch(self):
        shapes = []
        for (blocks, tiles), copies in zip(self.sizes, self.copies):
            shapes.append(pltpu.VMEM((blocks, tiles, 16, 128), F32))
            shapes.append(pltpu.VMEM((blocks, tiles, 16, 128), BF))
            shapes.append(pltpu.VMEM((copies, tiles, 16, 128), BF))
        if self.gathered:
            shapes.append(pltpu.VMEM((self.held, 16, 128), F32))
            shapes.append(pltpu.VMEM((3 if self.first == "x" else 1, self.held, 16, 128), F32))
        return shapes


PARTS = (Part(1, 0, 9, "zyx"), Part(2, 0, 9, "yzx"), Part(0, 0, 5, "zyx"), Part(0, 5, 4, "yzx"),)
ORDER = ((0, 0), (1, 0), (2, 0), (3, 0), (0, 1), (1, 1), (2, 1), (3, 1), (0, 2), (2, 2), (3, 2), (1, 2))
DURING = {(0, 0): 0, (1, 0): 1, (0, 2): 3}
SUMS = 4 * len(PARTS)


def kernel(scale, vol_hbm, w_hbm, ct_hbm, sw_ref, vg_ref, kg_ref, *rest):
    (
        vol, w, ct, spread, taps, tt, ttr, gp, gps, gpr, hs, hr, ps, pr, cr, swb, crossed, fine, vg, own,
        in_sem, out_sem, pair_ss, pair_rs, edge_ss, edge_rs, sw_ss, sw_rs, sum_ss, sum_rs, ready,
    ) = rest[:31]
    rest, room = list(rest[31:]), {}
    for i, part in enumerate(PARTS):
        count = len(part.scratch())
        room[i], rest = rest[:count], rest[count:]

    dp, sp = lax.axis_index("dp"), lax.axis_index("space")
    core, z, y, x = dp % 2, (dp // 2) % 4, (sp // 4) * 2 + dp // 8, sp % 4
    y_hi = sp // 4

    def chip(x, y, z, core):
        return ((y % 2) * 8 + z * 2 + core, (y // 2) * 4 + x)

    partner = chip(x, y, z, 1 - core)
    along = {
        "z": [chip(x, y, (z + j) % 4, core) for j in (1, 2, 3)],
        "y": [chip(x, (y + j) % 4, z, core) for j in (1, 2, 3)],
        "x": [chip((x + j) % 4, y, z, core) for j in (1, 2, 3)],
    }
    slabs = [(dp, (sp + j) % 8) for j in range(1, 8)]
    above, below = (dp, (sp + 1) % 8), (dp, (sp + 7) % 8)

    def remote(src, dst, ss, rs, to):
        return pltpu.make_async_remote_copy(
            src_ref=src, dst_ref=dst, send_sem=ss, recv_sem=rs, device_id=to, device_id_type=MESH
        )

    def signal(sem, to):
        pl.semaphore_signal(sem, inc=1, device_id=to, device_id_type=MESH)

    def landed(ref, sem):
        pltpu.make_async_copy(ref, ref, sem).wait()

    barrier = pltpu.get_barrier_semaphore()
    near = [along[axis][j] for axis in "xyz" for j in (0, 2)]
    for peer in [partner, *near]:
        signal(barrier, peer)

    @pl.when(sp == 3)
    def _():
        signal(barrier, above)

    @pl.when(sp == 4)
    def _():
        signal(barrier, below)

    loads = {}
    for i, p in enumerate((3, 0, 1, 2)):
        loads["v", p] = pltpu.make_async_copy(vol_hbm.at[p], vol.at[p], in_sem.at[i])
    for kd in range(3):
        rows = pl.ds(kd * 1152, 1152)
        loads["w", kd] = pltpu.make_async_copy(w_hbm.at[rows], w.at[rows], in_sem.at[4 + kd])
    loads["c"] = pltpu.make_async_copy(ct_hbm, ct, in_sem.at[7])
    for which in (("v", 3), ("w", 0), ("v", 0), ("v", 1), ("w", 1), ("w", 2), ("v", 2), "c"):
        loads[which].start()

    def edge(condition, ref):
        @pl.when(condition)
        def _():
            ref[...] = jnp.zeros(ref.shape, ref.dtype)

    edge(sp == 7, gp.at[2])
    edge(sp == 0, hr)

    first_column = lax.broadcasted_iota(jnp.int32, (512, 128), 0) % 16 == 0
    last_column = lax.broadcasted_iota(jnp.int32, (256, 256), 0) % 16 == 15

    def unfold(p):
        loads["v", p].wait()
        spread[pl.ds(8, 1024)] = vol[p].astype(F32)
        even = spread[pl.ds(8, 512, stride=2)].astype(BF)
        odd = spread[pl.ds(9, 512, stride=2)].astype(BF)
        left = jnp.where(first_column, 0.0, spread[pl.ds(7, 512, stride=2)]).astype(BF)
        for kw, source in enumerate((left, even, odd)):
            rows = source.reshape(16, 32, 128)
            upper, lower = rows[:, :16], rows[:, 16:]
            before = jnp.concatenate([jnp.zeros((1, 16, 128), BF), lower[:-1]], axis=0)
            for kh, block in enumerate((before, upper, lower)):
                at = (kh * 3 + kw) * 128
                taps[p, :, at : at + 128] = block.reshape(256, 128)

    row = lax.broadcasted_iota(jnp.int32, (128, 128), 0)
    column = lax.broadcasted_iota(jnp.int32, (128, 128), 1)
    channel = (((row % 64) // 8) * 2 + row // 64) * 8 + row % 8
    sort = (column == channel).astype(F32).astype(BF)

    def turn(p):
        for t in range(TAPS):
            turned = nt(sort, taps[p, :, t * 128 : (t + 1) * 128]).astype(BF)
            tt[0, p, t * 64 : (t + 1) * 64] = turned[:64]
            tt[1, p, t * 64 : (t + 1) * 64] = turned[64:]
        remote(tt.at[1 - core, p], ttr.at[p], pair_ss.at[3], pair_rs.at[3], partner).start()

    er = lax.broadcasted_iota(jnp.int32, (256, 256), 0)
    ec = lax.broadcasted_iota(jnp.int32, (256, 256), 1)
    unit = (er == ec).astype(F32).astype(BF)

    def share(o):
        return remote(gp.at[o], gpr.at[o], pair_ss.at[o], pair_rs.at[o], partner)

    def to_right(o):
        value = gp[o].astype(F32)
        gps[o] = jnp.where(last_column, 0.0, pltpu.roll(value, 255, 0)).astype(BF)

    def slope_of(v):
        s = jax.nn.sigmoid(v)
        return s, s * (1.0 + v * (1.0 - s))

    def finish(o, v):
        s, slope = slope_of(v)
        gp[o] = (ct[pl.ds(o * 256, 256)].astype(F32) * slope).astype(BF)
        swb[o] = nt(unit, (v * s).astype(BF)).astype(BF)

    def grad_plane(p):
        for half, moves in ((0, ((1, 0),)), (1, ((2, 0), (0, 1)))):
            lhs, lhs_right, rhs, rhs_right = [], [], [], []
            for o, kd in REACH[p]:
                for kh, down in moves:
                    for source, out in ((gp, lhs), (gps, lhs_right)):
                        value = source[o]
                        if down:
                            value = jnp.concatenate([value[16:], jnp.zeros((16, 256), BF)], axis=0)
                        out.append(value)
                    at = (kd * 9 + kh * 3) * 128
                    rhs_right.append(w[at : at + 128])
                    rhs.append(w[at + 128 : at + 384])
            both = nt(jnp.concatenate(lhs, axis=1), jnp.concatenate(rhs, axis=1))
            more = nt(jnp.concatenate(lhs_right, axis=1), jnp.concatenate(rhs_right, axis=1))
            fine[:, pl.ds(half * 32, 16, stride=2), :] = both[:, :128].reshape(16, 16, 128)
            fine[:, pl.ds(half * 32 + 1, 16, stride=2), :] = (both[:, 128:] + more).reshape(16, 16, 128)
        vg[p] = fine[:, 0:64].reshape(1024, 128).astype(BF)
        pltpu.make_async_copy(vg.at[p], vg_ref.at[p], out_sem.at[0]).start()

    def own_part(kd):
        (a, oa), (b, ob) = PAIRS[kd]
        lhs = jnp.concatenate([tt[core, a], tt[core, b]], axis=1)
        own[kd] = mm(lhs, jnp.concatenate([gp[oa], gp[ob]], axis=0))

    def pair_part(kd):
        (a, oa), (b, ob) = PAIRS[kd]
        lhs = jnp.concatenate([ttr[a], ttr[b]], axis=1)
        return mm(lhs, jnp.concatenate([gpr[oa], gpr[ob]], axis=0))

    place = {"x": x, "y": y, "z": z}
    across = [chip((x + j) % 4, (y + 2) % 4, z, core) for j in range(4)]

    def copies(i, stage):
        part, refs, out = PARTS[i], room[i], []
        at = i * 4 + stage
        if stage == 3:
            return [
                remote(refs[9], refs[10].at[j], sum_ss.at[at], sum_rs.at[at], to)
                for j, to in enumerate(along["x"] if part.first == "x" else along["y"][1:2])
            ]
        axis, blocks = part.axes[stage], part.sizes[stage][0]
        peers = along[axis] + (across if part.copies[stage] == 7 else [])
        for j, to in enumerate(peers):
            src = refs[3 * stage + 1].at[(place[axis] + j + 1) % blocks]
            out.append(remote(src, refs[3 * stage + 2].at[j], sum_ss.at[at], sum_rs.at[at], to))
        return out

    def arrived(i, stage, sems):
        landed(room[i][10 if stage == 3 else 3 * stage + 2], sems.at[i * 4 + stage])

    def send(i, stage):
        for c in reversed(copies(i, stage)):
            c.start()

    def put(i, total):
        part, refs = PARTS[i], room[i]
        for t in range(part.count):
            for group in range(8):
                at = (part.low + t) * 64 + group * 8
                tile = jnp.concatenate([total[at : at + 8, :128], total[at : at + 8, 128:]], axis=0)
                half = tile.astype(BF)
                y_lo, to_z = group // 4, group % 4
                for n, start in enumerate(part.starts):
                    k = t - start
                    if not 0 <= k < part.held:
                        continue
                    if part.first == "z":
                        block, where = to_z, y_lo * part.held + k
                    elif part.first == "y":
                        block, where = n * 2 + y_lo, to_z * part.held + k
                    else:
                        block, where = n, (to_z * 2 + y_lo) * part.held + k
                    refs[0][block, where] = tile
                    refs[1][block, where] = half
        send(i, 0)

    def put_all(kd, total):
        for i, part in enumerate(PARTS):
            if part.kd == kd:
                put(i, total)

    def write(part, owner, value):
        stride = part.starts[1] if len(part.starts) > 1 else 0
        value = value * scale
        for t in range(part.held):
            at = pl.multiple_of((part.kd * 9 + part.low + owner * stride + t) * 8, 8)
            kg_ref[pl.ds(at, 8), 0:128] = value[t, 0:8]
            kg_ref[pl.ds(at, 8), 128:256] = value[t, 8:16]

    def step(i, stage):
        part, refs = PARTS[i], room[i]
        arrived(i, stage, sum_rs)
        if stage == 3:
            if part.first == "y":
                write(part, 1 - y_hi, refs[10][0])
            else:
                for j in range(3):
                    write(part, (x + 3 - j) % 4, refs[10][j])
            return
        kept, _, got = refs[3 * stage : 3 * stage + 3]
        total = kept[place[part.axes[stage]] % part.sizes[stage][0]]
        for j in range(3):
            total = total + got[j].astype(F32)
        if stage < 2:
            total = total.reshape(*part.sizes[stage + 1], 16, 128)
            refs[3 * stage + 3][...] = total
            refs[3 * stage + 4][...] = total.astype(BF)
            send(i, stage + 1)
            return
        if part.gathered:
            refs[9][...] = total
            send(i, 3)
        write(part, {"z": 0, "y": y_hi, "x": x}[part.first], total)
        if part.copies[2] == 7:
            other = got[3].astype(F32)
            for j in (4, 5, 6):
                other = other + got[j].astype(F32)
            write(part, 1 - y_hi, other)

    other_row = along["y"][1]
    crossings = []

    def cells(slab, o):
        return pl.ds(pl.multiple_of(slab * 512 + o * 256, 256), 256)

    def hand_out(rows_of, slab, o):
        for j in range(4):
            rows = pl.ds(pl.multiple_of((x + j) % 4 * 32, 32), 32)
            src, dst = rows_of.at[rows], sw_ref.at[:, cells(slab, o)]
            if j == 0:
                pltpu.make_async_copy(src, dst, out_sem.at[1]).start()
            else:
                remote(src, dst, sw_ss.at[2], sw_rs.at[2], along["x"][j - 1]).start()

    def switch(o):
        rows = pl.ds(pl.multiple_of((1 - y_hi) * 128, 128), 128)
        crossings.append(remote(swb.at[o, rows], crossed.at[o], sw_ss.at[o], sw_rs.at[o], other_row))
        crossings[-1].start()
        rows = pl.ds(pl.multiple_of(y_hi * 128, 128), 128)
        hand_out(swb.at[o, rows], sp, o)

    def switch_on():
        for o, crossing in zip((1, 0), crossings):
            crossing.wait_recv()
            hand_out(crossed.at[o], (1 - y_hi) * 4 + x, o)

    spread[0:8] = jnp.zeros((8, 128), F32)
    unfold(3)
    loads["w", 0].wait()
    hs[...] = mm(taps[3], w[0:1152]).astype(BF)

    pl.semaphore_wait(barrier, 7 + jnp.where((sp == 3) | (sp == 4), 1, 0))
    halo = remote(hs, hr, edge_ss.at[0], edge_rs.at[0], above)
    slope_part = remote(ps, pr, edge_ss.at[1], edge_rs.at[1], below)
    slope_ct = remote(ct_hbm.at[pl.ds(0, 256)], cr, edge_ss.at[2], edge_rs.at[2], below)

    @pl.when(sp < 7)
    def _():
        halo.start()

    @pl.when(sp > 0)
    def _():
        slope_ct.start()

    for peer in near:
        signal(ready, peer)

    unfold(0)
    unfold(1)
    loads["w", 1].wait()
    loads["w", 2].wait()
    pre0 = mm(taps[0], w[1152:2304]) + mm(taps[1], w[2304:3456])
    ps[...] = pre0.astype(BF)

    @pl.when(sp > 0)
    def _():
        slope_part.start()

    turn(3)
    turn(1)
    turn(0)
    unfold(2)
    turn(2)
    pre1 = mm(taps[1], w[0:1152]) + mm(taps[2], w[1152:2304]) + mm(taps[3], w[2304:3456])
    loads["c"].wait()
    finish(1, pre1)
    share(1).start()
    pl.semaphore_wait(ready, len(near))
    switch(1)
    to_right(1)

    @pl.when(sp > 0)
    def _():
        halo.wait_recv()

    finish(0, pre0 + hr[...].astype(F32))
    share(0).start()
    switch(0)

    own_part(1)
    own_part(2)
    landed(ttr, pair_rs.at[3])
    share(1).wait_recv()
    share(0).wait_recv()
    total1 = own[1] + pair_part(1)
    put_all(1, total1)
    total2 = own[2] + pair_part(2)
    put_all(2, total2)

    @pl.when(sp < 7)
    def _():
        slope_ct.wait_recv()
        slope_part.wait_recv()
        _, slope = slope_of(pr[...].astype(F32) + hs[...].astype(F32))
        gp[2] = (cr[...].astype(F32) * slope).astype(BF)

    share(2).start()
    own_part(0)
    grad_plane(2)
    share(2).wait_recv()
    total0 = own[0] + pair_part(0)
    put_all(0, total0)
    to_right(0)
    to_right(2)
    for i, stage in ORDER:
        if (i, stage) in DURING:
            grad_plane(DURING[i, stage])
        step(i, stage)
        if (i, stage) == (0, 0):
            switch_on()

    landed(vg, out_sem.at[0])
    landed(sw_ref.at[:, pl.ds(0, 1024)], out_sem.at[1])
    landed(sw_ref.at[:, pl.ds(0, 3072)], sw_rs.at[2])
    landed(sw_ref.at[:, pl.ds(0, 3072)], sw_ss.at[2])
    for c in crossings:
        c.wait_send()
    landed(ttr, pair_ss.at[3])
    for o in range(3):
        share(o).wait_send()
    for i, stage in ORDER:
        arrived(i, stage, sum_ss)

    @pl.when(sp < 7)
    def _():
        halo.wait_send()

    @pl.when(sp > 0)
    def _():
        slope_ct.wait_send()
        slope_part.wait_send()


def deliver(sw_in, vg_in, kg_in, sw_out, vg_out, kg_out, sem):
    moves = [(kg_in, kg_out), (sw_in, sw_out)]
    moves += [(vg_in.at[p], vg_out.at[p]) for p in range(4)]
    moves = [pltpu.make_async_copy(a, b, sem.at[i]) for i, (a, b) in enumerate(moves)]
    for move in moves:
        move.start()
    for move in moves:
        move.wait()


RESULTS = (((32, 4096), BF), ((4, 1024, 128), BF), ((216, 256), F32))


def body(volume, weights, cotangent):
    count = 16 * 16 * 16 * 16
    vmem = pltpu.VMEM
    dma = pltpu.SemaphoreType.DMA
    whole = pl.BlockSpec(memory_space=pltpu.VMEM)
    far = pl.BlockSpec(memory_space=pltpu.HBM)
    anywhere = pl.BlockSpec(memory_space=pl.ANY)
    results = pl.pallas_call(
        functools.partial(kernel, 1.0 / count**0.5),
        out_shape=tuple(pltpu.VMEM(shape, dtype) for shape, dtype in RESULTS),
        in_specs=[far] * 3,
        out_specs=(anywhere, anywhere, whole),
        scratch_shapes=[
            vmem((4, 1024, 128), BF),
            vmem((3456, 256), BF),
            vmem((512, 256), BF),
            vmem((1040, 128), F32),
            vmem((4, 256, 1152), BF),
            vmem((2, 4, 576, 256), BF),
            vmem((4, 576, 256), BF),
            vmem((3, 256, 256), BF),
            vmem((3, 256, 256), BF),
            vmem((3, 256, 256), BF),
            vmem((256, 256), BF),
            vmem((256, 256), BF),
            vmem((256, 256), BF),
            vmem((256, 256), BF),
            vmem((256, 256), BF),
            vmem((2, 256, 256), BF),
            vmem((2, 128, 256), BF),
            vmem((16, 72, 128), F32),
            vmem((4, 1024, 128), BF),
            vmem((3, 576, 256), F32),
            dma((8,)),
            dma((2,)),
            dma((4,)),
            dma((4,)),
            dma((3,)),
            dma((3,)),
            dma((3,)),
            dma((3,)),
            dma((SUMS,)),
            dma((SUMS,)),
            pltpu.SemaphoreType.REGULAR,
            *[shape for part in PARTS for shape in part.scratch()],
        ],
        compiler_params=pltpu.CompilerParams(
            collective_id=0, has_side_effects=True, vmem_limit_bytes=40 * 2**20
        ),
        name="conv_step",
    )(
        *(
            pltpu.with_memory_space_constraint(value, pltpu.HBM)
            for value in (
                volume.reshape(4, 1024, 128),
                weights.reshape(3456, 256),
                cotangent.reshape(512, 256),
            )
        )
    )
    switched, volume_grad, kernel_grad = pl.pallas_call(
        deliver,
        out_shape=tuple(jax.ShapeDtypeStruct(shape, dtype) for shape, dtype in RESULTS),
        in_specs=[anywhere] * 3,
        out_specs=[far] * 3,
        scratch_shapes=[dma((6,))],
        compiler_params=pltpu.CompilerParams(vmem_limit_bytes=8 * 2**20),
        name="deliver",
    )(*results)
    return (
        switched[None],
        volume_grad.reshape(1, 4, 32, 32, 128),
        kernel_grad.reshape(3, 3, 3, 8, 256),
    )


def solution(mesh):
    in_specs = (P("dp", "space", None, None, None), P(), P("dp", "space", None, None, None))
    out_specs = (
        P("dp", "space", None),
        P("dp", "space", None, None, None),
        P(None, None, None, "dp", None),
    )
    return jax.shard_map(body, mesh=mesh, in_specs=in_specs, out_specs=out_specs, check_vma=False)
```
